32 devices in a mesh: row: 4 (over x, core), col: 8 (over z, y).
Axes of the slice: x: 2, y: 2, z: 4, core: 2. Of those that a mesh axis runs over, the one named last changes fastest.
Arguments:
- jump: float32 [3, 256, 1024], P(None, 'row', 'col'), may hold values from -6 to 6
- external: float32 [3, 256, 1024], P(None, 'row', 'col'), may hold values from -12 to 12
- cohesive: float32 [256, 1024], P('row', 'col'), may hold values from 0.5 to 4
- bond_mask: int32 [2, 256, 1024], P(None, 'row', 'col'), may hold values 0 or 1
- load_factor: float32 [1], replicated, may hold values from 0.5 to 1.5
- arc_radius: float32 [1], replicated, may hold values from 0.5 to 1.5
- stiffness: bfloat16 [1536, 1536], replicated, may hold values from -1 to 2
- coupling: float32 [3, 1536], replicated, may hold values from -6 to 6
- old_state: float32 [5120, 1536], P(('row', 'col')), may hold values from -3 to 3
- old_history: float32 [5120, 1536], P(('row', 'col')), may hold values from 0 to 1.5
- newton_steps: int32 [5120], P(('row', 'col')), may hold values from 0 to 9, as said below
- point_ids: int32 [5120], P(('row', 'col')), may hold values from 0 to 8191, as said below
Outputs:
- new_jump: float32 [3, 256, 1024], P(None, 'row', 'col')
- new_load: float32 [1], replicated
- new_state: float32 [2560, 1536], P(('row', 'col'))
- new_history: float32 [2560, 1536], P(('row', 'col'))
The draws below stay inside these ranges and needn't reach their ends.
Inputs may be any that keep to these rules, and one draw needn't show every extreme that they name: `newton_steps`: within one block the live slots number between 20 and 160, and some block has all 160 live; in all at most 2240 slots are live; a live slot's count is at least 2. `point_ids`: the slots of one block name distinct points of that block.
All inputs are finite; a program needn't handle non-finite values. No bound on the sum of `bond_mask` on one device may be relied on, other than what follows from the above.
Results may differ from the reference program's by a relative error of at most 0.0028.
Values sent between devices are 32-bit elements; how exact they have to be, the bound alone decides.
A program may use at most 64 MiB of HBM per device.

```python
import math
import jax
import jax.numpy as jnp
from jax import lax

CELLS = 1536
S_CAP = 160
PX = 64
PY = 128
MAX_STEPS = 9
SWEEPS = 3
NEW_CAP = 80
GX = 256
GY = 1024
SLOTS = 5120
NEW_SLOTS = 2560
N_ROW = 4
N_COL = 8


def draw_stiffness(key, part):
    first, second = jax.random.split(jax.random.fold_in(key, 11))
    noise = jax.random.normal(first, (CELLS, CELLS), jnp.float32) * (0.3 / math.sqrt(CELLS))
    symmetric = (noise + noise.T) / math.sqrt(2.0)
    leading = jax.random.uniform(second, (CELLS,), jnp.float32, 1.0, 2.0)
    identity = jnp.eye(CELLS, dtype=jnp.float32)
    return (symmetric * (1.0 - identity) + identity * leading[None, :]).astype(jnp.bfloat16)


def draw_external(key, part):
    shape = (3, GX, GY)
    position = jnp.arange(GX, dtype=jnp.float32)[None, :, None] / GX
    inner = jax.random.fold_in(key, 17)
    rough = jnp.clip(jax.random.normal(inner, shape, jnp.float32), -4.0, 4.0)
    return rough * (1.0 + 2.0 * position)


def draw_newton_steps(key, part):
    blocks = SLOTS // S_CAP
    order_key, size_key, place_key, step_key = jax.random.split(jax.random.fold_in(key, 29), 4)
    order = jax.random.permutation(order_key, blocks)
    crowded = order < blocks // 4
    sparse = jax.random.randint(size_key, (blocks,), S_CAP // 8, S_CAP // 4 + 1)
    held = jnp.where(crowded, S_CAP, sparse)

    def arrange(inner):
        return jax.random.permutation(inner, S_CAP)
    places = jax.vmap(arrange)(jax.random.split(place_key, blocks))
    occupied = places < held[:, None]
    counts = jax.random.randint(step_key, (blocks, S_CAP), 2, MAX_STEPS + 1)
    return jnp.where(occupied, counts, 0).reshape(SLOTS).astype(jnp.int32)


def draw_point_ids(key, part):
    blocks = SLOTS // S_CAP

    def choose(inner):
        return jax.random.permutation(inner, PX * PY)[:S_CAP]
    keys = jax.random.split(jax.random.fold_in(key, 31), blocks)
    return jax.vmap(choose)(keys).reshape(SLOTS).astype(jnp.int32)


def set_ends(values, stream_key, least, largest):
    extent = values.shape
    place = [jax.random.randint(jax.random.fold_in(stream_key, axis), (), 0, extent[axis]) for axis in range(len(extent))]
    values = values.at[tuple(place)].set(least)
    longest = extent.index(max(extent))
    place[longest] = (place[longest] + 1) % extent[longest]
    return values.at[tuple(place)].set(largest)


def block_levels(own_key, dims, cuts, least, top_value):
    def one(dim, shards_of):
        steps = jax.random.uniform(jax.random.fold_in(jax.random.fold_in(own_key, 6), dim), (shards_of,), jnp.float32, least / len(cuts), top_value / len(cuts))
        return jnp.repeat(jnp.exp(steps), dims[dim] // shards_of).reshape((-1,) + (1,) * (len(dims) - dim - 1))

    loudness = one(*cuts[0])
    for cut in cuts[1:]:
        loudness = loudness * one(*cut)
    return loudness


def scatter_about(stream_key, shape, spread, limit, pieces=(), kind=jnp.bfloat16):
    values = jax.random.normal(stream_key, shape, jnp.float32) * spread
    if len(pieces) > 0:
        values = block_levels(stream_key, shape, pieces, -0.22, 0.18) * values
    return jnp.clip(values, min=-limit, max=limit).astype(kind)


def setup_inputs(seed: int = 0) -> dict:
    streams_of = jax.random.split(jax.random.key(seed), 13)
    return {
        "jump": scatter_about(streams_of[0], (3, GX, GY), 1.0, 6.0, ((1, 4), (2, 8)), jnp.float32),
        "external": draw_external(jax.random.fold_in(streams_of[12], 71), 0),
        "cohesive": jnp.clip(jnp.exp(math.log(4.0) - 2.0794415 * jax.random.uniform(streams_of[2], (GX, GY), jnp.float32) ** block_levels(streams_of[2], (GX, GY), ((0, 4), (1, 8)), -0.2, 0.2)), 0.5, 4.0),
        "bond_mask": set_ends((jax.random.randint(streams_of[3], (2, GX, GY), 0, 4) < 3).astype(jnp.int32), jax.random.fold_in(streams_of[3], 1), 0, 1),
        "load_factor": jnp.clip(jax.random.uniform(streams_of[4], (1,), jnp.float32, 0.5, 1.5), 0.5, 1.5),
        "arc_radius": jnp.clip(jax.random.uniform(streams_of[5], (1,), jnp.float32, 0.5, 1.5), 0.5, 1.5),
        "stiffness": draw_stiffness(jax.random.fold_in(streams_of[12], 71), 0),
        "coupling": scatter_about(streams_of[7], (3, CELLS), 1.0, 6.0, (), jnp.float32),
        "old_state": scatter_about(streams_of[8], (SLOTS, CELLS), 0.5, 3.0, ((0, 32),), jnp.float32),
        "old_history": jnp.clip(1.5 * jax.random.uniform(streams_of[9], (SLOTS, CELLS), jnp.float32) ** block_levels(streams_of[9], (SLOTS, CELLS), ((0, 32),), -0.2, 0.2), 0.0, 1.5),
        "newton_steps": draw_newton_steps(jax.random.fold_in(streams_of[12], 71), 0),
        "point_ids": draw_point_ids(jax.random.fold_in(streams_of[12], 71), 0),
    }


softening = 1.0

def micro_solve(state, history, drive, steps, stiffness, coupling):
    diagonal = jnp.diagonal(stiffness).astype(jnp.float32)
    load = jnp.dot(drive, coupling, precision=lax.Precision.HIGHEST)
    damage = jnp.exp(-history)

    def advance(count, current):
        bent = jnp.tanh(current)
        force = jnp.dot(current.astype(jnp.bfloat16), stiffness, preferred_element_type=jnp.float32)
        misfit = force + softening * damage * bent - load
        slope = diagonal + softening * damage * (1.0 - bent * bent)
        return jnp.where((count < steps)[:, None], current - misfit / slope, current)
    state = lax.fori_loop(0, MAX_STEPS, advance, state)
    bent = jnp.tanh(state)
    cells = state.shape[1]
    traction = jnp.dot(softening * damage * bent, coupling.T, precision=lax.Precision.HIGHEST) / cells
    weight = softening * damage * (1.0 - bent * bent)
    products = jnp.stack([coupling[0] * coupling[0], coupling[1] * coupling[1], coupling[2] * coupling[2], coupling[0] * coupling[1], coupling[0] * coupling[2], coupling[1] * coupling[2]])
    tangent = jnp.dot(weight, products.T, precision=lax.Precision.HIGHEST) / cells
    history = jnp.maximum(history, jnp.abs(state))
    return (state, history, traction, tangent)

def block_solve(scale, tangent, source):
    d00 = scale + tangent[0]
    d11 = scale + tangent[1]
    d22 = scale + tangent[2]
    d01, d02, d12 = (tangent[3], tangent[4], tangent[5])
    c00 = d11 * d22 - d12 * d12
    c11 = d00 * d22 - d02 * d02
    c22 = d00 * d11 - d01 * d01
    c01 = d02 * d12 - d01 * d22
    c02 = d01 * d12 - d02 * d11
    c12 = d01 * d02 - d00 * d12
    determinant = d00 * c00 + d01 * c01 + d02 * c02
    first = (c00 * source[0] + c01 * source[1] + c02 * source[2]) / determinant
    second = (c01 * source[0] + c11 * source[1] + c12 * source[2]) / determinant
    third = (c02 * source[0] + c12 * source[1] + c22 * source[2]) / determinant
    return jnp.stack([first, second, third])

def neighbours(field, bond_x, low_x, bond_y, low_y):
    padded = jnp.pad(field, ((0, 0), (1, 1), (1, 1)))
    return bond_x * padded[:, 2:, 1:-1] + low_x * padded[:, :-2, 1:-1] + bond_y * padded[:, 1:-1, 2:] + low_y * padded[:, 1:-1, :-2]

def reference(jump, external, cohesive, bond_mask, load_factor, arc_radius, stiffness, coupling, old_state, old_history, newton_steps, point_ids):
    devices = N_ROW * N_COL
    slot_block = jnp.arange(SLOTS, dtype=jnp.int32) // S_CAP
    grid_x = slot_block // N_COL * PX + point_ids // PY
    grid_y = slot_block % N_COL * PY + point_ids % PY
    drive = jump[:, grid_x, grid_y].T
    live = newton_steps > 0
    live_float = live.astype(jnp.float32)

    def per_block(block):
        return micro_solve(block[0], block[1], block[2], block[3], stiffness, coupling)
    blocks = (old_state.reshape(devices, S_CAP, CELLS), old_history.reshape(devices, S_CAP, CELLS), drive.reshape(devices, S_CAP, 3), newton_steps.reshape(devices, S_CAP))
    state, history, traction, tangent = lax.map(per_block, blocks)
    state = state.reshape(SLOTS, CELLS)
    history = history.reshape(SLOTS, CELLS)
    traction = traction.reshape(SLOTS, 3)
    tangent = tangent.reshape(SLOTS, 6)
    soft = jnp.zeros((GX, GY), jnp.float32).at[grid_x, grid_y].add(live_float)
    rve_traction = jnp.zeros((3, GX, GY), jnp.float32).at[:, grid_x, grid_y].add((traction * live_float[:, None]).T)
    rve_tangent = jnp.zeros((6, GX, GY), jnp.float32).at[:, grid_x, grid_y].add((tangent * live_float[:, None]).T)
    bond_x = 0.25 + 0.75 * bond_mask[0].astype(jnp.float32)
    bond_y = 0.25 + 0.75 * bond_mask[1].astype(jnp.float32)
    low_x = jnp.pad(bond_x, ((1, 0), (0, 0)))[:-1]
    low_y = jnp.pad(bond_y, ((0, 0), (1, 0)))[:, :-1]
    scale = bond_x + low_x + bond_y + low_y + (1.0 - soft) * cohesive
    residual = scale * jump - neighbours(jump, bond_x, low_x, bond_y, low_y) + rve_traction - load_factor[0] * external
    source = jnp.concatenate([-residual, external])

    def solve_both(values):
        return jnp.concatenate([block_solve(scale, rve_tangent, values[:3]), block_solve(scale, rve_tangent, values[3:])])
    iterate = solve_both(source)
    for sweep in range(SWEEPS):
        iterate = solve_both(source + neighbours(iterate, bond_x, low_x, bond_y, low_y))
    correction, direction = (iterate[:3], iterate[3:])
    cross = jnp.sum(correction * direction)
    square = jnp.sum(direction * direction)
    entries = 3.0 * GX * GY
    shifted = square + 0.25 * entries
    increment = (arc_radius[0] * jnp.sqrt(entries) * jnp.sqrt(shifted) - cross) / shifted
    new_jump = jump + correction + increment * direction
    new_load = load_factor + increment
    live_int = live.astype(jnp.int32)
    rank = jnp.cumsum(live_int, dtype=jnp.int32) - live_int
    home_block = rank // 2 % devices
    home_slot = 2 * (rank // (2 * devices)) + rank % 2
    target = jnp.where(live, home_block * NEW_CAP + home_slot, NEW_SLOTS).astype(jnp.int32)
    new_state = jnp.zeros((NEW_SLOTS, CELLS), jnp.float32).at[target].set(state, mode='drop')
    new_history = jnp.zeros((NEW_SLOTS, CELLS), jnp.float32).at[target].set(history, mode='drop')
    return (new_jump, new_load, new_state, new_history)
```

```python
import functools

import jax
import jax.numpy as jnp
from jax import lax
from jax.experimental import pallas as pl
from jax.experimental.pallas import tpu as pltpu
from jax.sharding import PartitionSpec as P

MAX_STEPS = 9
SWEEPS = 3
TILE = 256
EARLY = 1
CHUNKS = (5, 13, 22)
LANES = 128
MESH = pl.DeviceIdType.MESH
F32 = jnp.float32
BF16 = jnp.bfloat16


def iota(shape, dim):
    return lax.broadcasted_iota(jnp.int32, shape, dim)


def picked(onehot, values):
    high = values.astype(BF16)
    rest = values - high.astype(F32)
    middle = rest.astype(BF16)
    low = (rest - middle.astype(F32)).astype(BF16)
    dot = functools.partial(jnp.dot, preferred_element_type=F32)
    return dot(onehot, high) + dot(onehot, middle) + dot(onehot, low)


def body(
    nrow,
    ncol,
    pair,
    direct,
    jump_hbm,
    external_hbm,
    cohesive_hbm,
    bond_hbm,
    load_hbm,
    radius_hbm,
    coupling_hbm,
    steps_hbm,
    points_hbm,
    stiffness_hbm,
    state_hbm,
    history_hbm,
    new_jump_ref,
    new_load_ref,
    new_state_ref,
    new_history_ref,
    jump_ref,
    external_ref,
    cohesive_ref,
    bond_ref,
    load_ref,
    radius_ref,
    coupling_ref,
    steps_ref,
    points_ref,
    stiff,
    state,
    history,
    damage,
    load,
    rounded,
    diagonal,
    count_out,
    count_in,
    sum_out,
    sum_in,
    x_out,
    x_in,
    y_out,
    y_in,
    out_history,
    in_history,
    out_state,
    in_state,
    local_sems,
    halo_send,
    halo_recv,
    all_send,
    all_recv,
):
    devices = nrow * ncol
    row, col = lax.axis_index("row"), lax.axis_index("col")
    here = row * ncol + col
    slots, cells = state.shape
    X, Y = cohesive_ref.shape
    new_cap = new_state_ref.shape[0]
    padded = out_history.shape[1]
    width = devices * padded
    bits = devices.bit_length() - 1

    half = devices // 2
    side = lax.div(row, nrow // 2)

    names = (
        (steps_hbm, steps_ref),
        (jump_hbm, jump_ref),
        (bond_hbm, bond_ref),
        (points_hbm, points_ref),
        (coupling_hbm, coupling_ref),
        (history_hbm, history),
        (stiffness_hbm, stiff),
        (state_hbm, state),
        (external_hbm, external_ref),
        (cohesive_hbm, cohesive_ref),
        (load_hbm, load_ref),
        (radius_hbm, radius_ref),
    )
    fetch = []
    for index, (source, target) in enumerate(names):
        fetch.append(pltpu.make_async_copy(source, target, local_sems.at[index]))
        fetch[-1].start()

    def locate(p):
        return {"row": lax.div(p, ncol), "col": lax.rem(p, ncol)}

    def peer(k):
        p = lax.rem(here + k, devices)
        return locate(p), p

    x_in[...] = jnp.zeros_like(x_in)
    y_in[...] = jnp.zeros_like(y_in)

    barrier = pltpu.get_barrier_semaphore()

    def greet(k, carry):
        device, _ = peer(k)
        pl.semaphore_signal(barrier, inc=1, device_id=device, device_id_type=MESH)
        return carry

    lax.fori_loop(1, devices, greet, 0)

    if pair < padded:
        blank = jnp.zeros((devices, padded - pair, cells), F32)
        in_history[:, pair:, :] = blank
        in_state[:, pair:, :] = blank

    fetch[0].wait()
    steps_row = steps_ref[...]
    live_row = (steps_row > 0).astype(F32)
    count_out[...] = jnp.broadcast_to(jnp.sum(live_row, axis=1, keepdims=True), count_out.shape)

    lane = iota((X, Y), 1)
    line = iota((X, Y), 0)

    def stage(phase, fields):
        edges = jnp.zeros((X, Y), F32)
        for c, (x_field, y_field) in enumerate(fields):
            x_out[phase, 0, c : c + 1, :] = x_field[X - 1 : X, :]
            x_out[phase, 1, c : c + 1, :] = x_field[0:1, :]
            edges = jnp.where(lane == c, pltpu.roll(y_field, (c + 1) % Y, 1), edges)
            edges = jnp.where(lane == c + 8, pltpu.roll(y_field, c + 8, 1), edges)
        turned_edges = jnp.concatenate([edges, jnp.zeros((Y - X, Y), F32)], axis=0).T
        y_out[phase, 0] = turned_edges[0:8, :]
        y_out[phase, 1] = turned_edges[8:16, :]

    def edges_of(phase):
        both = [y_in[phase, 0], y_in[phase, 1], jnp.zeros((Y - 16, Y), F32)]
        return jnp.concatenate(both, axis=0).T[:X, :]

    def halo_copies(phase):
        plan = (
            (x_out, x_in, 0, row < nrow - 1, row > 0, {"row": row + 1, "col": col}),
            (x_out, x_in, 1, row > 0, row < nrow - 1, {"row": row - 1, "col": col}),
            (y_out, y_in, 0, col < ncol - 1, col > 0, {"row": row, "col": col + 1}),
            (y_out, y_in, 1, col > 0, col < ncol - 1, {"row": row, "col": col - 1}),
        )
        copies = []
        for index, (source, target, way, sends, gets, device) in enumerate(plan):
            copy = pltpu.make_async_remote_copy(
                src_ref=source.at[phase, way],
                dst_ref=target.at[phase, way],
                send_sem=halo_send.at[phase, index],
                recv_sem=halo_recv.at[phase, index],
                device_id=device,
                device_id_type=MESH,
            )
            copies.append((copy, sends, gets))
        return copies

    def halo_start(phase):
        for copy, sends, _ in halo_copies(phase):
            pl.when(sends)(copy.start)

    def halo_wait(phase):
        for copy, sends, gets in halo_copies(phase):
            pl.when(gets)(copy.wait_recv)

    def halo_wait_sends(phase):
        for copy, sends, gets in halo_copies(phase):
            pl.when(sends)(copy.wait_send)

    def send(source, target, kind, device):
        pltpu.make_async_remote_copy(
            src_ref=source,
            dst_ref=target,
            send_sem=all_send.at[kind],
            recv_sem=all_recv.at[kind],
            device_id=device,
            device_id_type=MESH,
        ).start()

    def spread(source_of, target, kind, first, last):
        def one(k, carry):
            device, p = peer(k)
            send(source_of(p), target, kind, device)
            return carry

        lax.fori_loop(first, last, one, 0)

    def spread_wait(buffer, sem):
        pltpu.make_async_copy(buffer, buffer, sem).wait()

    direct_part = pl.ds(0, direct)
    shared_part = pl.ds(direct, pair - direct)

    def send_shared(out, inside, kind):
        if direct == pair:
            return

        def one(k, carry):
            p = side * half + lax.rem(lax.rem(here, half) + k, half)
            send(out.at[p, shared_part], inside.at[here, shared_part], kind, locate(p))
            return carry

        lax.fori_loop(1, half, one, 0)

    def send_direct(out, inside, kind, first, last):
        spread(
            lambda p: out.at[p, direct_part], inside.at[here, direct_part], kind, first, last
        )

    def forward(inside, kind):
        if direct == pair:
            return
        spread_wait(inside.at[pl.ds(0, half - 1), shared_part], all_recv.at[kind])
        mine = inside.at[pl.ds(side * half, half), shared_part]
        send(mine, mine, kind + 2, locate(lax.rem(here + half, devices)))

    def rows_wait(inside, kind):
        spread_wait(inside.at[pl.ds(0, devices - 1), direct_part], all_recv.at[kind + 1])
        if direct < pair:
            spread_wait(inside.at[pl.ds(0, half), shared_part], all_recv.at[kind + 2])

    def sends_wait(inside, kind):
        spread_wait(inside.at[pl.ds(0, devices - 1), direct_part], all_send.at[kind + 1])
        if direct < pair:
            spread_wait(inside.at[pl.ds(0, half - 1), shared_part], all_send.at[kind])
            spread_wait(inside.at[pl.ds(0, half), shared_part], all_send.at[kind + 2])

    fetch[1].wait()
    fetch[2].wait()
    bond_x = 0.25 + 0.75 * bond_ref[0].astype(F32)
    bond_y = 0.25 + 0.75 * bond_ref[1].astype(F32)
    jump = [jump_ref[c] for c in range(3)]
    stage(0, [(jump[c], jump[c]) for c in range(3)] + [(bond_x, bond_y)])

    pl.semaphore_wait(barrier, devices - 1)

    count_in[pl.ds(here, 1)] = count_out[...][None]
    spread(lambda p: count_out, count_in.at[here], 0, 1, devices)
    halo_start(0)

    fetch[3].wait()
    slot_line = iota((slots, slots), 0)
    slot_lane = iota((slots, slots), 1)

    def to_column(values):
        return jnp.sum(jnp.where(slot_line == slot_lane, values, 0.0), axis=1, keepdims=True)

    points_row = points_ref[...]
    px_row = lax.shift_right_logical(points_row, (Y.bit_length() - 1))
    py_row = points_row & (Y - 1)
    px_col = to_column(px_row.astype(F32)).astype(jnp.int32)
    py_col = to_column(py_row.astype(F32)).astype(jnp.int32)
    steps_col = to_column(steps_row.astype(F32)).astype(jnp.int32)
    live_col = (steps_col > 0).astype(F32)
    at_x = (iota((slots, X), 1) == px_col).astype(F32).astype(BF16)
    at_y = (iota((slots, Y), 1) == py_col).astype(F32)
    at_x_turned = (iota((X, slots), 0) == px_row).astype(F32).astype(BF16)
    fetch[4].wait()
    drive = []
    for c in range(3):
        lines = picked(at_x, jump[c])
        drive.append(jnp.sum(lines * at_y, axis=1, keepdims=True))
    for start in range(0, cells, TILE):
        part = slice(start, start + TILE)
        total = drive[0] * coupling_ref[0:1, part]
        total = total + drive[1] * coupling_ref[1:2, part]
        load[:, part] = total + drive[2] * coupling_ref[2:3, part]
    rank_row = jnp.sum(jnp.where(slot_line < slot_lane, live_col, 0.0), axis=0, keepdims=True)

    fetch[5].wait()
    for start in range(0, cells, TILE):
        part = slice(start, start + TILE)
        damage[:, part] = jnp.exp(-history[:, part])

    fetch[6].wait()
    fetch[7].wait()
    tile_eye = iota((TILE, TILE), 0) == iota((TILE, TILE), 1)
    for start in range(0, cells, TILE):
        part = slice(start, start + TILE)
        block = stiff[part, part].astype(F32)
        diagonal[:, part] = jnp.sum(jnp.where(tile_eye, block, 0.0), axis=0, keepdims=True)
        rounded[0, :, part] = state[:, part].astype(BF16)

    def advance(count, carry):
        now = lax.rem(count, 2)
        moves = count < steps_col
        for start in range(0, cells, TILE):
            part = slice(start, start + TILE)
            force = jnp.dot(rounded[now], stiff[:, part], preferred_element_type=F32)
            current = state[:, part]
            bent = jnp.tanh(current)
            worn = damage[:, part]
            misfit = force + worn * bent - load[:, part]
            slope = diagonal[:, part] + worn * (1.0 - bent * bent)
            current = jnp.where(moves, current - misfit / slope, current)
            state[:, part] = current
            rounded[1 - now, :, part] = current.astype(BF16)
        return carry

    lax.fori_loop(0, EARLY, advance, 0)

    spread_wait(count_in.at[pl.ds(0, devices - 1)], all_recv.at[0])
    counts = count_in[:, 0, :]
    device_line = iota((devices, LANES), 0)
    device_lane = iota((devices, LANES), 1)
    starts = jnp.sum(jnp.where(device_line < device_lane, counts, 0.0), axis=0, keepdims=True)
    ends = jnp.sum(jnp.where(device_line <= device_lane, counts, 0.0), axis=0, keepdims=True)
    my_start = jnp.sum(jnp.where(device_line < here, counts, 0.0), axis=0, keepdims=True)[:, :1]
    my_start = my_start.astype(jnp.int32)

    def place(rank, first):
        pairs = lax.shift_right_logical(rank, 1) - lax.shift_right_logical(first, 1)
        spot = 2 * lax.shift_right_logical(pairs, bits) + (rank & 1)
        if direct == pair:
            return spot
        spot = spot - jnp.where((pairs & (devices - 1)) == 0, first & 1, 0)
        return jnp.where(spot < direct, spot, direct + (rank & 1))

    ranks = rank_row.astype(jnp.int32) + my_start
    home = lax.shift_right_logical(ranks, 1) & (devices - 1)
    spots = place(ranks, my_start)
    if direct < pair:
        home = jnp.where(spots < direct, home, (home & (half - 1)) + side * half)
    leaves = jnp.where(steps_row > 0, home * padded + spots, -1)
    leaving = (iota((width, slots), 0) == leaves).astype(F32).astype(BF16)

    wanted_slot = iota((new_cap, LANES), 0)
    wanted = 2 * (here + devices * lax.shift_right_logical(wanted_slot, 1)) + (wanted_slot & 1)
    wanted_lane = iota((new_cap, LANES), 1)
    wanted_float = wanted.astype(F32)
    hit = (starts <= wanted_float) & (wanted_float < ends) & (wanted_lane < devices)
    valid = jnp.sum(jnp.where(hit, 1.0, 0.0), axis=1, keepdims=True)
    from_start = jnp.sum(jnp.where(hit, starts, 0.0), axis=1, keepdims=True).astype(jnp.int32)
    source = jnp.sum(jnp.where(hit, wanted_lane.astype(F32), 0.0), axis=1, keepdims=True)
    arrives = source.astype(jnp.int32) * padded + place(wanted[:, :1], from_start)
    arrives = jnp.where(valid > 0.0, arrives, -1)
    coming = (iota((new_cap, width), 1) == arrives).astype(F32).astype(BF16)

    def gather_out(values, out, inside):
        for start in range(0, cells, TILE):
            part = slice(start, start + TILE)
            rows = picked(leaving, values[:, part])
            out[:, :, part] = rows.reshape(devices, padded, TILE)
        inside[pl.ds(here, 1)] = out[pl.ds(here, 1)]

    gather_out(history, out_history, in_history)
    send_shared(out_history, in_history, 1)
    send_direct(out_history, in_history, 2, 1, devices)

    lax.fori_loop(EARLY, MAX_STEPS, advance, 0)

    others = devices - 1
    bounds = [1] + [1 + others * s // 31 for s in CHUNKS] + [devices]

    gather_out(state, out_state, in_state)

    def send_state(step):
        if step == 0:
            send_shared(out_state, in_state, 4)
        send_direct(out_state, in_state, 5, bounds[step], bounds[step + 1])

    first_sum = jnp.zeros((slots, 16), F32)
    second_sum = jnp.zeros((slots, 16), F32)
    turned = (((1,), (1,)), ((), ()))

    def split(values):
        high = values.astype(BF16)
        return high, (values - high.astype(F32)).astype(BF16)

    def summed(values, factors):
        high, low = split(values)
        both = factors.astype(BF16).astype(F32)
        both = jnp.concatenate([both, factors - both], axis=0).astype(BF16)
        dot = functools.partial(
            lax.dot_general, dimension_numbers=turned, preferred_element_type=F32
        )
        return dot(high, both) + dot(low, both)

    for start in range(0, cells, TILE):
        part = slice(start, start + TILE)
        bent = jnp.tanh(state[:, part])
        worn = damage[:, part]
        a0, a1, a2 = [coupling_ref[a : a + 1, part] for a in range(3)]
        none = jnp.zeros((2, TILE), F32)
        firsts = jnp.concatenate([a0, a1, a2, none, none, none[:1]], axis=0)
        seconds = jnp.concatenate(
            [a0 * a0, a1 * a1, a2 * a2, a0 * a1, a0 * a2, a1 * a2, none], axis=0
        )
        first_sum = first_sum + summed(worn * bent, firsts)
        second_sum = second_sum + summed(worn * (1.0 - bent * bent), seconds)
    first_sum = (first_sum[:, :8] + first_sum[:, 8:]) * (live_col / cells)
    second_sum = (second_sum[:, :8] + second_sum[:, 8:]) * (live_col / cells)

    def put(values):
        return picked(at_x_turned, at_y * values)

    soft = put(live_col)
    rve_traction = [put(first_sum[:, c : c + 1]) for c in range(3)]
    tangent = [put(second_sum[:, c : c + 1]) for c in range(6)]

    halo_wait(0)
    for copy in fetch[8:]:
        copy.wait()

    def before_x(phase, field, c):
        return jnp.where(line == 0, x_in[phase, 0, c : c + 1, :], pltpu.roll(field, 1, 0))

    def after_x(phase, field, c):
        return jnp.where(line == X - 1, x_in[phase, 1, c : c + 1, :], pltpu.roll(field, X - 1, 0))

    def before_y(edges, field, c):
        edge = pltpu.roll(edges, (Y - c) % Y, 1)
        return jnp.where(lane == 0, edge, pltpu.roll(field, 1, 1))

    def after_y(edges, field, c):
        edge = pltpu.roll(edges, Y - 9 - c, 1)
        return jnp.where(lane == Y - 1, edge, pltpu.roll(field, Y - 1, 1))

    low_x = before_x(0, bond_x, 3)
    first_edges = edges_of(0)
    low_y = before_y(first_edges, bond_y, 3)

    def neighbours(phase, edges, field, c):
        return (
            bond_x * after_x(phase, field, c)
            + low_x * before_x(phase, field, c)
            + bond_y * after_y(edges, field, c)
            + low_y * before_y(edges, field, c)
        )

    scale = bond_x + low_x + bond_y + low_y + (1.0 - soft) * cohesive_ref[...]
    load_factor = load_ref[...]
    terms = []
    for c in range(3):
        residual = (
            scale * jump[c]
            - neighbours(0, first_edges, jump[c], c)
            + rve_traction[c]
            - load_factor * external_ref[c]
        )
        terms.append(-residual)
    for c in range(3):
        terms.append(external_ref[c])
    d00, d11, d22 = [scale + tangent[c] for c in range(3)]
    d01, d02, d12 = tangent[3:]
    c00 = d11 * d22 - d12 * d12
    c11 = d00 * d22 - d02 * d02
    c22 = d00 * d11 - d01 * d01
    c01 = d02 * d12 - d01 * d22
    c02 = d01 * d12 - d02 * d11
    c12 = d01 * d02 - d00 * d12
    inverse = 1.0 / (d00 * c00 + d01 * c01 + d02 * c02)
    c00, c11, c22, c01, c02, c12 = [c * inverse for c in (c00, c11, c22, c01, c02, c12)]

    def solve_both(w):
        result = []
        for h in (0, 3):
            result.append(c00 * w[h] + c01 * w[h + 1] + c02 * w[h + 2])
            result.append(c01 * w[h] + c11 * w[h + 1] + c12 * w[h + 2])
            result.append(c02 * w[h] + c12 * w[h + 1] + c22 * w[h + 2])
        return result

    iterate = solve_both(terms)
    peers = pl.ds(0, devices - 1)
    for sweep in range(SWEEPS):
        phase = sweep + 1
        stage(phase, [(v, v) for v in iterate])
        halo_start(phase)
        if sweep == 0:
            forward(in_history, 1)
        send_state(sweep)
        if sweep == 1:
            rows_wait(in_history, 1)
            for start in range(0, cells, TILE):
                part = slice(start, start + TILE)
                kept = picked(coming, in_history[:, :, part].reshape(width, TILE))
                new_history_ref[:, part] = kept
        if sweep == 2:
            forward(in_state, 4)
        halo_wait(phase)
        edges = edges_of(phase)
        iterate = solve_both([terms[c] + neighbours(phase, edges, iterate[c], c) for c in range(6)])
    correction, direction = iterate[:3], iterate[3:]

    def total_of(fields):
        return jnp.sum(fields[0] + fields[1] + fields[2], axis=0, keepdims=True)

    cross_row = total_of([correction[c] * direction[c] for c in range(3)])
    square_row = total_of([direction[c] * direction[c] for c in range(3)])
    own_cross = jnp.sum(cross_row, axis=1, keepdims=True)
    own_square = jnp.sum(square_row, axis=1, keepdims=True)
    sum_out[...] = jnp.where(iota((1, Y), 1) == 0, own_cross, own_square)
    sum_in[pl.ds(here, 1)] = sum_out[...][None]
    spread(lambda p: sum_out, sum_in.at[here], 7, 1, devices)
    send_state(SWEEPS)
    spread_wait(sum_in.at[pl.ds(0, devices - 1)], all_recv.at[7])
    sums = jnp.sum(sum_in[...], axis=0)
    cross = sums[:, 0:1]
    square = sums[:, 1:2]
    entries = 3.0 * X * Y * devices
    shifted = square + 0.25 * entries
    root = jnp.sqrt(shifted) * (entries**0.5)
    increment = (radius_ref[...] * root - cross) / shifted
    for c in range(3):
        new_jump_ref[c] = jump[c] + correction[c] + increment * direction[c]
    new_load_ref[...] = load_factor + increment

    rows_wait(in_state, 4)
    for start in range(0, cells, TILE):
        part = slice(start, start + TILE)
        moved = picked(coming, in_state[:, :, part].reshape(width, TILE))
        new_state_ref[:, part] = moved
        new_history_ref[:, part] = jnp.maximum(new_history_ref[:, part], jnp.abs(moved))

    for phase in range(SWEEPS + 1):
        halo_wait_sends(phase)
    spread_wait(count_in.at[peers], all_send.at[0])
    sends_wait(out_history, 1)
    sends_wait(out_state, 4)
    spread_wait(sum_in.at[peers], all_send.at[7])


def on_device(
    jump,
    external,
    cohesive,
    bond_mask,
    load_factor,
    arc_radius,
    stiffness,
    coupling,
    old_state,
    old_history,
    newton_steps,
    point_ids,
):
    nrow, ncol = lax.axis_size("row"), lax.axis_size("col")
    devices = nrow * ncol
    slots, cells = old_state.shape
    X, Y = cohesive.shape
    new_cap = slots // 2
    pair = 2 * ((slots + 2 * devices + 1) // (2 * devices))
    padded = 8 * ((pair + 7) // 8)
    phases = SWEEPS + 1
    shares = pair > 2 and nrow % 2 == 0 and slots <= (pair - 1) * devices
    direct = pair - 2 if shares else pair
    vmem = pl.BlockSpec(memory_space=pltpu.VMEM)
    hbm = pl.BlockSpec(memory_space=pltpu.HBM)
    new_jump, new_load, new_state, new_history = pl.pallas_call(
        functools.partial(body, nrow, ncol, pair, direct),
        out_shape=(
            jax.ShapeDtypeStruct(jump.shape, F32),
            jax.ShapeDtypeStruct((1, 1), F32),
            jax.ShapeDtypeStruct((new_cap, cells), F32),
            jax.ShapeDtypeStruct((new_cap, cells), F32),
        ),
        in_specs=[hbm] * 12,
        out_specs=(vmem,) * 4,
        scratch_shapes=[
            pltpu.VMEM(jump.shape, F32),
            pltpu.VMEM(external.shape, F32),
            pltpu.VMEM(cohesive.shape, F32),
            pltpu.VMEM(bond_mask.shape, jnp.int32),
            pltpu.VMEM((1, 1), F32),
            pltpu.VMEM((1, 1), F32),
            pltpu.VMEM(coupling.shape, F32),
            pltpu.VMEM((1, slots), jnp.int32),
            pltpu.VMEM((1, slots), jnp.int32),
            pltpu.VMEM((cells, cells), BF16),
            pltpu.VMEM((slots, cells), F32),
            pltpu.VMEM((slots, cells), F32),
            pltpu.VMEM((slots, cells), F32),
            pltpu.VMEM((slots, cells), F32),
            pltpu.VMEM((2, slots, cells), BF16),
            pltpu.VMEM((1, cells), F32),
            pltpu.VMEM((1, LANES), F32),
            pltpu.VMEM((devices, 1, LANES), F32),
            pltpu.VMEM((1, Y), F32),
            pltpu.VMEM((devices, 1, Y), F32),
            pltpu.VMEM((phases, 2, 8, Y), F32),
            pltpu.VMEM((phases, 2, 8, Y), F32),
            pltpu.VMEM((phases, 2, 8, Y), F32),
            pltpu.VMEM((phases, 2, 8, Y), F32),
            pltpu.VMEM((devices, padded, cells), F32),
            pltpu.VMEM((devices, padded, cells), F32),
            pltpu.VMEM((devices, padded, cells), F32),
            pltpu.VMEM((devices, padded, cells), F32),
            pltpu.SemaphoreType.DMA((12,)),
            pltpu.SemaphoreType.DMA((phases, 4)),
            pltpu.SemaphoreType.DMA((phases, 4)),
            pltpu.SemaphoreType.DMA((8,)),
            pltpu.SemaphoreType.DMA((8,)),
        ],
        compiler_params=pltpu.CompilerParams(
            collective_id=0, has_side_effects=True, vmem_limit_bytes=60 * 1024 * 1024
        ),
    )(
        jump,
        external,
        cohesive,
        bond_mask,
        load_factor.reshape(1, 1),
        arc_radius.reshape(1, 1),
        coupling,
        newton_steps.reshape(1, slots),
        point_ids.reshape(1, slots),
        stiffness,
        old_state,
        old_history,
    )
    return new_jump, new_load.reshape(1), new_state, new_history


def solution(mesh):
    in_specs = (
        P(None, "row", "col"),
        P(None, "row", "col"),
        P("row", "col"),
        P(None, "row", "col"),
        P(),
        P(),
        P(),
        P(),
        P(("row", "col"), None),
        P(("row", "col"), None),
        P(("row", "col")),
        P(("row", "col")),
    )
    out_specs = (P(None, "row", "col"), P(), P(("row", "col"), None), P(("row", "col"), None))
    return jax.shard_map(
        on_device, mesh=mesh, in_specs=in_specs, out_specs=out_specs, check_vma=False
    )
```

```python
import functools

import jax
import jax.numpy as jnp
from jax import lax
from jax.experimental import pallas as pl
from jax.experimental.pallas import tpu as pltpu
from jax.sharding import PartitionSpec as P

MAX_STEPS = 9
SWEEPS = 3
TILE = 256
EARLY = 1
GRANT = 60 * 1024 * 1024
CHUNKS = (5, 13, 22)
LANES = 128
MESH = pl.DeviceIdType.MESH
F32 = jnp.float32
BF16 = jnp.bfloat16


def iota(shape, dim):
    return lax.broadcasted_iota(jnp.int32, shape, dim)


def picked(onehot, values):
    high = values.astype(BF16)
    rest = values - high.astype(F32)
    middle = rest.astype(BF16)
    low = (rest - middle.astype(F32)).astype(BF16)
    dot = functools.partial(jnp.dot, preferred_element_type=F32)
    return dot(onehot, high) + dot(onehot, middle) + dot(onehot, low)


def body(
    nrow,
    ncol,
    pair,
    direct,
    jump_hbm,
    external_hbm,
    cohesive_hbm,
    bond_hbm,
    load_hbm,
    radius_hbm,
    coupling_hbm,
    steps_hbm,
    points_hbm,
    stiffness_hbm,
    state_hbm,
    history_hbm,
    new_jump_ref,
    new_load_ref,
    new_state_ref,
    new_history_ref,
    jump_ref,
    external_ref,
    cohesive_ref,
    bond_ref,
    load_ref,
    radius_ref,
    coupling_ref,
    steps_ref,
    points_ref,
    stiff,
    state,
    history,
    damage,
    load,
    rounded,
    diagonal,
    count_out,
    count_in,
    sum_out,
    sum_in,
    x_out,
    x_in,
    y_out,
    y_in,
    out_history,
    in_history,
    out_state,
    in_state,
    local_sems,
    halo_send,
    halo_recv,
    all_send,
    all_recv,
):
    devices = nrow * ncol
    row, col = lax.axis_index("row"), lax.axis_index("col")
    here = row * ncol + col
    slots, cells = state.shape
    X, Y = cohesive_ref.shape
    new_cap = new_state_ref.shape[0]
    padded = out_history.shape[1]
    width = devices * padded
    bits = devices.bit_length() - 1

    half = devices // 2
    side = lax.div(row, nrow // 2)

    names = (
        (steps_hbm, steps_ref),
        (jump_hbm, jump_ref),
        (bond_hbm, bond_ref),
        (points_hbm, points_ref),
        (coupling_hbm, coupling_ref),
        (history_hbm, history),
        (stiffness_hbm, stiff),
        (state_hbm, state),
        (external_hbm, external_ref),
        (cohesive_hbm, cohesive_ref),
        (load_hbm, load_ref),
        (radius_hbm, radius_ref),
    )
    fetch = []
    for index, (source, target) in enumerate(names):
        fetch.append(pltpu.make_async_copy(source, target, local_sems.at[index]))
        fetch[-1].start()

    def locate(p):
        return {"row": lax.div(p, ncol), "col": lax.rem(p, ncol)}

    def peer(k):
        p = lax.rem(here + k, devices)
        return locate(p), p

    x_in[...] = jnp.zeros_like(x_in)
    y_in[...] = jnp.zeros_like(y_in)

    barrier = pltpu.get_barrier_semaphore()

    def greet(k, carry):
        device, _ = peer(k)
        pl.semaphore_signal(barrier, inc=1, device_id=device, device_id_type=MESH)
        return carry

    lax.fori_loop(1, devices, greet, 0)

    if pair < padded:
        blank = jnp.zeros((devices, padded - pair, cells), F32)
        in_history[:, pair:, :] = blank
        in_state[:, pair:, :] = blank

    fetch[0].wait()
    steps_row = steps_ref[...]
    live_row = (steps_row > 0).astype(F32)
    count_out[...] = jnp.broadcast_to(jnp.sum(live_row, axis=1, keepdims=True), count_out.shape)

    lane = iota((X, Y), 1)
    line = iota((X, Y), 0)

    def stage(phase, fields):
        edges = jnp.zeros((X, Y), F32)
        for c, (x_field, y_field) in enumerate(fields):
            x_out[phase, 0, c : c + 1, :] = x_field[X - 1 : X, :]
            x_out[phase, 1, c : c + 1, :] = x_field[0:1, :]
            edges = jnp.where(lane == c, pltpu.roll(y_field, (c + 1) % Y, 1), edges)
            edges = jnp.where(lane == c + 8, pltpu.roll(y_field, c + 8, 1), edges)
        turned_edges = jnp.concatenate([edges, jnp.zeros((Y - X, Y), F32)], axis=0).T
        y_out[phase, 0] = turned_edges[0:8, :]
        y_out[phase, 1] = turned_edges[8:16, :]

    def edges_of(phase):
        both = [y_in[phase, 0], y_in[phase, 1], jnp.zeros((Y - 16, Y), F32)]
        return jnp.concatenate(both, axis=0).T[:X, :]

    def halo_copies(phase):
        plan = (
            (x_out, x_in, 0, row < nrow - 1, row > 0, {"row": row + 1, "col": col}),
            (x_out, x_in, 1, row > 0, row < nrow - 1, {"row": row - 1, "col": col}),
            (y_out, y_in, 0, col < ncol - 1, col > 0, {"row": row, "col": col + 1}),
            (y_out, y_in, 1, col > 0, col < ncol - 1, {"row": row, "col": col - 1}),
        )
        copies = []
        for index, (source, target, way, sends, gets, device) in enumerate(plan):
            copy = pltpu.make_async_remote_copy(
                src_ref=source.at[phase, way],
                dst_ref=target.at[phase, way],
                send_sem=halo_send.at[phase, index],
                recv_sem=halo_recv.at[phase, index],
                device_id=device,
                device_id_type=MESH,
            )
            copies.append((copy, sends, gets))
        return copies

    def halo_start(phase):
        for copy, sends, _ in halo_copies(phase):
            pl.when(sends)(copy.start)

    def halo_wait(phase):
        for copy, sends, gets in halo_copies(phase):
            pl.when(gets)(copy.wait_recv)

    def halo_wait_sends(phase):
        for copy, sends, gets in halo_copies(phase):
            pl.when(sends)(copy.wait_send)

    def send(source, target, kind, device):
        pltpu.make_async_remote_copy(
            src_ref=source,
            dst_ref=target,
            send_sem=all_send.at[kind],
            recv_sem=all_recv.at[kind],
            device_id=device,
            device_id_type=MESH,
        ).start()

    def spread(source_of, target, kind, first, last):
        def one(k, carry):
            device, p = peer(k)
            send(source_of(p), target, kind, device)
            return carry

        lax.fori_loop(first, last, one, 0)

    def spread_wait(buffer, sem):
        pltpu.make_async_copy(buffer, buffer, sem).wait()

    direct_part = pl.ds(0, direct)
    shared_part = pl.ds(direct, pair - direct)

    def send_shared(out, inside, kind):
        if direct == pair:
            return

        def one(k, carry):
            p = side * half + lax.rem(lax.rem(here, half) + k, half)
            send(out.at[p, shared_part], inside.at[here, shared_part], kind, locate(p))
            return carry

        lax.fori_loop(1, half, one, 0)

    def send_direct(out, inside, kind, first, last):
        spread(
            lambda p: out.at[p, direct_part], inside.at[here, direct_part], kind, first, last
        )

    def forward(inside, kind):
        if direct == pair:
            return
        spread_wait(inside.at[pl.ds(0, half - 1), shared_part], all_recv.at[kind])
        mine = inside.at[pl.ds(side * half, half), shared_part]
        send(mine, mine, kind + 2, locate(lax.rem(here + half, devices)))

    def rows_wait(inside, kind):
        spread_wait(inside.at[pl.ds(0, devices - 1), direct_part], all_recv.at[kind + 1])
        if direct < pair:
            spread_wait(inside.at[pl.ds(0, half), shared_part], all_recv.at[kind + 2])

    def sends_wait(inside, kind):
        spread_wait(inside.at[pl.ds(0, devices - 1), direct_part], all_send.at[kind + 1])
        if direct < pair:
            spread_wait(inside.at[pl.ds(0, half - 1), shared_part], all_send.at[kind])
            spread_wait(inside.at[pl.ds(0, half), shared_part], all_send.at[kind + 2])

    fetch[1].wait()
    fetch[2].wait()
    bond_x = 0.25 + 0.75 * bond_ref[0].astype(F32)
    bond_y = 0.25 + 0.75 * bond_ref[1].astype(F32)
    jump = [jump_ref[c] for c in range(3)]
    stage(0, [(jump[c], jump[c]) for c in range(3)] + [(bond_x, bond_y)])

    pl.semaphore_wait(barrier, devices - 1)

    count_in[pl.ds(here, 1)] = count_out[...][None]
    spread(lambda p: count_out, count_in.at[here], 0, 1, devices)
    halo_start(0)

    fetch[3].wait()
    slot_line = iota((slots, slots), 0)
    slot_lane = iota((slots, slots), 1)

    def to_column(values):
        return jnp.sum(jnp.where(slot_line == slot_lane, values, 0.0), axis=1, keepdims=True)

    points_row = points_ref[...]
    px_row = lax.shift_right_logical(points_row, (Y.bit_length() - 1))
    py_row = points_row & (Y - 1)
    px_col = to_column(px_row.astype(F32)).astype(jnp.int32)
    py_col = to_column(py_row.astype(F32)).astype(jnp.int32)
    steps_col = to_column(steps_row.astype(F32)).astype(jnp.int32)
    live_col = (steps_col > 0).astype(F32)
    at_x = (iota((slots, X), 1) == px_col).astype(F32).astype(BF16)
    at_y = (iota((slots, Y), 1) == py_col).astype(F32)
    at_x_turned = (iota((X, slots), 0) == px_row).astype(F32).astype(BF16)
    fetch[4].wait()
    drive = []
    for c in range(3):
        lines = picked(at_x, jump[c])
        drive.append(jnp.sum(lines * at_y, axis=1, keepdims=True))
    for start in range(0, cells, TILE):
        part = slice(start, start + TILE)
        total = drive[0] * coupling_ref[0:1, part]
        total = total + drive[1] * coupling_ref[1:2, part]
        load[:, part] = total + drive[2] * coupling_ref[2:3, part]
    rank_row = jnp.sum(jnp.where(slot_line < slot_lane, live_col, 0.0), axis=0, keepdims=True)

    fetch[5].wait()
    for start in range(0, cells, TILE):
        part = slice(start, start + TILE)
        damage[:, part] = jnp.exp(-history[:, part])

    fetch[6].wait()
    fetch[7].wait()
    tile_eye = iota((TILE, TILE), 0) == iota((TILE, TILE), 1)
    for start in range(0, cells, TILE):
        part = slice(start, start + TILE)
        block = stiff[part, part].astype(F32)
        diagonal[:, part] = jnp.sum(jnp.where(tile_eye, block, 0.0), axis=0, keepdims=True)
        rounded[0, :, part] = state[:, part].astype(BF16)

    def advance(count, carry):
        now = lax.rem(count, 2)
        moves = count < steps_col
        for start in range(0, cells, TILE):
            part = slice(start, start + TILE)
            force = jnp.dot(rounded[now], stiff[:, part], preferred_element_type=F32)
            current = state[:, part]
            bent = jnp.tanh(current)
            worn = damage[:, part]
            misfit = force + worn * bent - load[:, part]
            slope = diagonal[:, part] + worn * (1.0 - bent * bent)
            current = jnp.where(moves, current - misfit / slope, current)
            state[:, part] = current
            rounded[1 - now, :, part] = current.astype(BF16)
        return carry

    lax.fori_loop(0, EARLY, advance, 0)

    spread_wait(count_in.at[pl.ds(0, devices - 1)], all_recv.at[0])
    counts = count_in[:, 0, :]
    device_line = iota((devices, LANES), 0)
    device_lane = iota((devices, LANES), 1)
    starts = jnp.sum(jnp.where(device_line < device_lane, counts, 0.0), axis=0, keepdims=True)
    ends = jnp.sum(jnp.where(device_line <= device_lane, counts, 0.0), axis=0, keepdims=True)
    my_start = jnp.sum(jnp.where(device_line < here, counts, 0.0), axis=0, keepdims=True)[:, :1]
    my_start = my_start.astype(jnp.int32)

    def place(rank, first):
        pairs = lax.shift_right_logical(rank, 1) - lax.shift_right_logical(first, 1)
        spot = 2 * lax.shift_right_logical(pairs, bits) + (rank & 1)
        if direct == pair:
            return spot
        spot = spot - jnp.where((pairs & (devices - 1)) == 0, first & 1, 0)
        return jnp.where(spot < direct, spot, direct + (rank & 1))

    ranks = rank_row.astype(jnp.int32) + my_start
    home = lax.shift_right_logical(ranks, 1) & (devices - 1)
    spots = place(ranks, my_start)
    if direct < pair:
        home = jnp.where(spots < direct, home, (home & (half - 1)) + side * half)
    leaves = jnp.where(steps_row > 0, home * padded + spots, -1)
    leaving = (iota((width, slots), 0) == leaves).astype(F32).astype(BF16)

    wanted_slot = iota((new_cap, LANES), 0)
    wanted = 2 * (here + devices * lax.shift_right_logical(wanted_slot, 1)) + (wanted_slot & 1)
    wanted_lane = iota((new_cap, LANES), 1)
    wanted_float = wanted.astype(F32)
    hit = (starts <= wanted_float) & (wanted_float < ends) & (wanted_lane < devices)
    valid = jnp.sum(jnp.where(hit, 1.0, 0.0), axis=1, keepdims=True)
    from_start = jnp.sum(jnp.where(hit, starts, 0.0), axis=1, keepdims=True).astype(jnp.int32)
    source = jnp.sum(jnp.where(hit, wanted_lane.astype(F32), 0.0), axis=1, keepdims=True)
    arrives = source.astype(jnp.int32) * padded + place(wanted[:, :1], from_start)
    arrives = jnp.where(valid > 0.0, arrives, -1)
    coming = (iota((new_cap, width), 1) == arrives).astype(F32).astype(BF16)

    def gather_out(values, out, inside):
        for start in range(0, cells, TILE):
            part = slice(start, start + TILE)
            rows = picked(leaving, values[:, part])
            out[:, :, part] = rows.reshape(devices, padded, TILE)
        inside[pl.ds(here, 1)] = out[pl.ds(here, 1)]

    gather_out(history, out_history, in_history)
    send_shared(out_history, in_history, 1)
    send_direct(out_history, in_history, 2, 1, devices)

    lax.fori_loop(EARLY, MAX_STEPS, advance, 0)

    others = devices - 1
    bounds = [1] + [1 + others * s // 31 for s in CHUNKS] + [devices]

    gather_out(state, out_state, in_state)

    def send_state(step):
        if step == 0:
            send_shared(out_state, in_state, 4)
        send_direct(out_state, in_state, 5, bounds[step], bounds[step + 1])

    first_sum = jnp.zeros((slots, 16), F32)
    second_sum = jnp.zeros((slots, 16), F32)
    turned = (((1,), (1,)), ((), ()))

    def split(values):
        high = values.astype(BF16)
        return high, (values - high.astype(F32)).astype(BF16)

    def summed(values, factors):
        high, low = split(values)
        both = factors.astype(BF16).astype(F32)
        both = jnp.concatenate([both, factors - both], axis=0).astype(BF16)
        dot = functools.partial(
            lax.dot_general, dimension_numbers=turned, preferred_element_type=F32
        )
        return dot(high, both) + dot(low, both)

    for start in range(0, cells, TILE):
        part = slice(start, start + TILE)
        bent = jnp.tanh(state[:, part])
        worn = damage[:, part]
        a0, a1, a2 = [coupling_ref[a : a + 1, part] for a in range(3)]
        none = jnp.zeros((2, TILE), F32)
        firsts = jnp.concatenate([a0, a1, a2, none, none, none[:1]], axis=0)
        seconds = jnp.concatenate(
            [a0 * a0, a1 * a1, a2 * a2, a0 * a1, a0 * a2, a1 * a2, none], axis=0
        )
        first_sum = first_sum + summed(worn * bent, firsts)
        second_sum = second_sum + summed(worn * (1.0 - bent * bent), seconds)
    first_sum = (first_sum[:, :8] + first_sum[:, 8:]) * (live_col / cells)
    second_sum = (second_sum[:, :8] + second_sum[:, 8:]) * (live_col / cells)

    def put(values):
        return picked(at_x_turned, at_y * values)

    soft = put(live_col)
    rve_traction = [put(first_sum[:, c : c + 1]) for c in range(3)]
    tangent = [put(second_sum[:, c : c + 1]) for c in range(6)]

    halo_wait(0)
    for copy in fetch[8:]:
        copy.wait()

    def before_x(phase, field, c):
        return jnp.where(line == 0, x_in[phase, 0, c : c + 1, :], pltpu.roll(field, 1, 0))

    def after_x(phase, field, c):
        return jnp.where(line == X - 1, x_in[phase, 1, c : c + 1, :], pltpu.roll(field, X - 1, 0))

    def before_y(edges, field, c):
        edge = pltpu.roll(edges, (Y - c) % Y, 1)
        return jnp.where(lane == 0, edge, pltpu.roll(field, 1, 1))

    def after_y(edges, field, c):
        edge = pltpu.roll(edges, Y - 9 - c, 1)
        return jnp.where(lane == Y - 1, edge, pltpu.roll(field, Y - 1, 1))

    low_x = before_x(0, bond_x, 3)
    first_edges = edges_of(0)
    low_y = before_y(first_edges, bond_y, 3)

    def neighbours(phase, edges, field, c):
        return (
            bond_x * after_x(phase, field, c)
            + low_x * before_x(phase, field, c)
            + bond_y * after_y(edges, field, c)
            + low_y * before_y(edges, field, c)
        )

    scale = bond_x + low_x + bond_y + low_y + (1.0 - soft) * cohesive_ref[...]
    load_factor = load_ref[0]
    terms = []
    for c in range(3):
        residual = (
            scale * jump[c]
            - neighbours(0, first_edges, jump[c], c)
            + rve_traction[c]
            - load_factor * external_ref[c]
        )
        terms.append(-residual)
    for c in range(3):
        terms.append(external_ref[c])
    d00, d11, d22 = [scale + tangent[c] for c in range(3)]
    d01, d02, d12 = tangent[3:]
    c00 = d11 * d22 - d12 * d12
    c11 = d00 * d22 - d02 * d02
    c22 = d00 * d11 - d01 * d01
    c01 = d02 * d12 - d01 * d22
    c02 = d01 * d12 - d02 * d11
    c12 = d01 * d02 - d00 * d12
    inverse = 1.0 / (d00 * c00 + d01 * c01 + d02 * c02)
    c00, c11, c22, c01, c02, c12 = [c * inverse for c in (c00, c11, c22, c01, c02, c12)]

    def solve_both(w):
        result = []
        for h in (0, 3):
            result.append(c00 * w[h] + c01 * w[h + 1] + c02 * w[h + 2])
            result.append(c01 * w[h] + c11 * w[h + 1] + c12 * w[h + 2])
            result.append(c02 * w[h] + c12 * w[h + 1] + c22 * w[h + 2])
        return result

    iterate = solve_both(terms)
    peers = pl.ds(0, devices - 1)
    for sweep in range(SWEEPS):
        phase = sweep + 1
        stage(phase, [(v, v) for v in iterate])
        halo_start(phase)
        if sweep == 0:
            forward(in_history, 1)
        send_state(sweep)
        if sweep == 1:
            rows_wait(in_history, 1)
            for start in range(0, cells, TILE):
                part = slice(start, start + TILE)
                kept = picked(coming, in_history[:, :, part].reshape(width, TILE))
                new_history_ref[:, part] = kept
        if sweep == 2:
            forward(in_state, 4)
        halo_wait(phase)
        edges = edges_of(phase)
        iterate = solve_both([terms[c] + neighbours(phase, edges, iterate[c], c) for c in range(6)])
    correction, direction = iterate[:3], iterate[3:]

    def total_of(fields):
        return jnp.sum(fields[0] + fields[1] + fields[2], axis=0, keepdims=True)

    cross_row = total_of([correction[c] * direction[c] for c in range(3)])
    square_row = total_of([direction[c] * direction[c] for c in range(3)])
    own_cross = jnp.sum(cross_row, axis=1, keepdims=True)
    own_square = jnp.sum(square_row, axis=1, keepdims=True)
    sum_out[...] = jnp.where(iota((1, Y), 1) == 0, own_cross, own_square)
    sum_in[pl.ds(here, 1)] = sum_out[...][None]
    spread(lambda p: sum_out, sum_in.at[here], 7, 1, devices)
    send_state(SWEEPS)
    spread_wait(sum_in.at[pl.ds(0, devices - 1)], all_recv.at[7])
    sums = jnp.sum(sum_in[...], axis=0)
    cross = sums[:, 0:1]
    square = sums[:, 1:2]
    entries = 3.0 * X * Y * devices
    shifted = square + 0.25 * entries
    root = jnp.sqrt(shifted) * (entries**0.5)
    increment = (radius_ref[0] * root - cross) / shifted
    for c in range(3):
        new_jump_ref[c] = jump[c] + correction[c] + increment * direction[c]
    new_load_ref[...] = load_factor + increment

    rows_wait(in_state, 4)
    for start in range(0, cells, TILE):
        part = slice(start, start + TILE)
        moved = picked(coming, in_state[:, :, part].reshape(width, TILE))
        new_state_ref[:, part] = moved

    for phase in range(SWEEPS + 1):
        halo_wait_sends(phase)
    spread_wait(count_in.at[peers], all_send.at[0])
    sends_wait(out_history, 1)
    sends_wait(out_state, 4)
    spread_wait(sum_in.at[peers], all_send.at[7])


def finish(jump_ref, load_ref, state_ref, history_ref, *outs):
    new_jump_ref, new_load_ref, new_state_ref, new_history_ref = outs
    new_jump_ref[...] = jump_ref[...]
    new_load_ref[...] = load_ref[...]
    new_state_ref[...] = state_ref[...]
    new_history_ref[...] = jnp.maximum(history_ref[...], jnp.abs(state_ref[...]))


def on_device(
    jump,
    external,
    cohesive,
    bond_mask,
    load_factor,
    arc_radius,
    stiffness,
    coupling,
    old_state,
    old_history,
    newton_steps,
    point_ids,
):
    nrow, ncol = lax.axis_size("row"), lax.axis_size("col")
    devices = nrow * ncol
    slots, cells = old_state.shape
    X, Y = cohesive.shape
    new_cap = slots // 2
    pair = 2 * ((slots + 2 * devices + 1) // (2 * devices))
    padded = 8 * ((pair + 7) // 8)
    phases = SWEEPS + 1
    shares = pair > 2 and nrow % 2 == 0 and slots <= (pair - 1) * devices
    direct = pair - 2 if shares else pair
    out_shape = (
        jax.ShapeDtypeStruct(jump.shape, F32),
        jax.ShapeDtypeStruct((1, 1), F32),
        jax.ShapeDtypeStruct((new_cap, cells), F32),
        jax.ShapeDtypeStruct((new_cap, cells), F32),
    )
    vmem = pl.BlockSpec(memory_space=pltpu.VMEM)
    hbm = pl.BlockSpec(memory_space=pltpu.HBM)
    results = pl.pallas_call(
        functools.partial(body, nrow, ncol, pair, direct),
        out_shape=out_shape,
        in_specs=[hbm] * 12,
        out_specs=(vmem,) * 4,
        scratch_shapes=[
            pltpu.VMEM(jump.shape, F32),
            pltpu.VMEM(external.shape, F32),
            pltpu.VMEM(cohesive.shape, F32),
            pltpu.VMEM(bond_mask.shape, jnp.int32),
            pltpu.SMEM((1,), F32),
            pltpu.SMEM((1,), F32),
            pltpu.VMEM(coupling.shape, F32),
            pltpu.VMEM((1, slots), jnp.int32),
            pltpu.VMEM((1, slots), jnp.int32),
            pltpu.VMEM((cells, cells), BF16),
            pltpu.VMEM((slots, cells), F32),
            pltpu.VMEM((slots, cells), F32),
            pltpu.VMEM((slots, cells), F32),
            pltpu.VMEM((slots, cells), F32),
            pltpu.VMEM((2, slots, cells), BF16),
            pltpu.VMEM((1, cells), F32),
            pltpu.VMEM((1, LANES), F32),
            pltpu.VMEM((devices, 1, LANES), F32),
            pltpu.VMEM((1, Y), F32),
            pltpu.VMEM((devices, 1, Y), F32),
            pltpu.VMEM((phases, 2, 8, Y), F32),
            pltpu.VMEM((phases, 2, 8, Y), F32),
            pltpu.VMEM((phases, 2, 8, Y), F32),
            pltpu.VMEM((phases, 2, 8, Y), F32),
            pltpu.VMEM((devices, padded, cells), F32),
            pltpu.VMEM((devices, padded, cells), F32),
            pltpu.VMEM((devices, padded, cells), F32),
            pltpu.VMEM((devices, padded, cells), F32),
            pltpu.SemaphoreType.DMA((12,)),
            pltpu.SemaphoreType.DMA((phases, 4)),
            pltpu.SemaphoreType.DMA((phases, 4)),
            pltpu.SemaphoreType.DMA((8,)),
            pltpu.SemaphoreType.DMA((8,)),
        ],
        compiler_params=pltpu.CompilerParams(
            collective_id=0, has_side_effects=True, vmem_limit_bytes=GRANT
        ),
    )(
        jump,
        external,
        cohesive,
        bond_mask,
        load_factor,
        arc_radius,
        coupling,
        newton_steps.reshape(1, slots),
        point_ids.reshape(1, slots),
        stiffness,
        old_state,
        old_history,
    )
    new_jump, new_load, new_state, new_history = pl.pallas_call(
        finish,
        out_shape=out_shape,
        in_specs=[vmem] * 4,
        out_specs=(vmem,) * 4,
        compiler_params=pltpu.CompilerParams(vmem_limit_bytes=GRANT),
    )(*results)
    return new_jump, new_load.reshape(1), new_state, new_history


def solution(mesh):
    in_specs = (
        P(None, "row", "col"),
        P(None, "row", "col"),
        P("row", "col"),
        P(None, "row", "col"),
        P(),
        P(),
        P(),
        P(),
        P(("row", "col"), None),
        P(("row", "col"), None),
        P(("row", "col")),
        P(("row", "col")),
    )
    out_specs = (P(None, "row", "col"), P(), P(("row", "col"), None), P(("row", "col"), None))
    return jax.shard_map(
        on_device, mesh=mesh, in_specs=in_specs, out_specs=out_specs, check_vma=False
    )
```

```python
import functools

import jax
import jax.numpy as jnp
from jax import lax
from jax.experimental import pallas as pl
from jax.experimental.pallas import tpu as pltpu
from jax.sharding import PartitionSpec as P

MAX_STEPS = 9
SWEEPS = 3
TILE = 256
WIDE = 768
EARLY = 1
GRANT = 60 * 1024 * 1024
CHUNKS = (4, 11, 19)
LANES = 128
MESH = pl.DeviceIdType.MESH
F32 = jnp.float32
BF16 = jnp.bfloat16


def iota(shape, dim):
    return lax.broadcasted_iota(jnp.int32, shape, dim)


def pieces_of(values):
    high = values.astype(BF16)
    rest = values - high.astype(F32)
    middle = rest.astype(BF16)
    low = (rest - middle.astype(F32)).astype(BF16)
    return high, middle, low


def joined(onehot, pieces):
    dot = functools.partial(jnp.dot, preferred_element_type=F32)
    return dot(onehot, pieces[0]) + dot(onehot, pieces[1]) + dot(onehot, pieces[2])


def picked(onehot, values):
    return joined(onehot, pieces_of(values))


def body(
    nrow,
    ncol,
    pair,
    direct,
    jump_hbm,
    external_hbm,
    cohesive_hbm,
    bond_hbm,
    load_hbm,
    radius_hbm,
    coupling_hbm,
    steps_hbm,
    points_hbm,
    stiffness_hbm,
    state_hbm,
    history_hbm,
    new_jump_hbm,
    new_load_hbm,
    coming_hbm,
    kept_hbm,
    in_state,
    new_jump_ref,
    new_load_ref,
    coming_ref,
    kept_ref,
    pieces,
    jump_ref,
    external_ref,
    cohesive_ref,
    bond_ref,
    load_ref,
    radius_ref,
    coupling_ref,
    steps_ref,
    points_ref,
    stiff,
    state,
    history,
    damage,
    load,
    rounded,
    diagonal,
    count_out,
    count_in,
    sum_out,
    sum_in,
    x_out,
    x_in,
    y_out,
    y_in,
    out_history,
    in_history,
    out_state,
    local_sems,
    result_sems,
    halo_send,
    halo_recv,
    all_send,
    all_recv,
):
    devices = nrow * ncol
    row, col = lax.axis_index("row"), lax.axis_index("col")
    here = row * ncol + col
    slots, cells = state.shape
    X, Y = cohesive_ref.shape
    new_cap = kept_ref.shape[0]
    padded = out_history.shape[1]
    width = devices * padded
    bits = devices.bit_length() - 1

    half = devices // 2
    side = lax.div(row, nrow // 2)

    names = (
        (steps_hbm, steps_ref),
        (jump_hbm, jump_ref),
        (bond_hbm, bond_ref),
        (points_hbm, points_ref),
        (coupling_hbm, coupling_ref),
        (history_hbm, history),
        (stiffness_hbm, stiff),
        (state_hbm, state),
        (external_hbm, external_ref),
        (cohesive_hbm, cohesive_ref),
        (load_hbm, load_ref),
        (radius_hbm, radius_ref),
    )
    fetch = []
    for index, (source, target) in enumerate(names):
        fetch.append(pltpu.make_async_copy(source, target, local_sems.at[index]))
    fetch[0].start()

    def locate(p):
        return {"row": lax.div(p, ncol), "col": lax.rem(p, ncol)}

    def peer(k):
        p = lax.rem(here + k, devices)
        return locate(p), p

    x_in[...] = jnp.zeros_like(x_in)
    y_in[...] = jnp.zeros_like(y_in)

    barrier = pltpu.get_barrier_semaphore()

    def greet(k, carry):
        device, _ = peer(k)
        pl.semaphore_signal(barrier, inc=1, device_id=device, device_id_type=MESH)
        return carry

    lax.fori_loop(1, devices, greet, 0)
    for copy in fetch[1:]:
        copy.start()

    if pair < padded:
        blank = jnp.zeros((devices, padded - pair, cells), F32)
        in_history[:, pair:, :] = blank

    fetch[0].wait()
    steps_row = steps_ref[...]
    live_row = (steps_row > 0).astype(F32)
    count_out[...] = jnp.broadcast_to(jnp.sum(live_row, axis=1, keepdims=True), count_out.shape)

    lane = iota((X, Y), 1)
    line = iota((X, Y), 0)

    def stage(phase, fields):
        edges = jnp.zeros((X, Y), F32)
        for c, (x_field, y_field) in enumerate(fields):
            x_out[phase, 0, c : c + 1, :] = x_field[X - 1 : X, :]
            x_out[phase, 1, c : c + 1, :] = x_field[0:1, :]
            edges = jnp.where(lane == c, pltpu.roll(y_field, (c + 1) % Y, 1), edges)
            edges = jnp.where(lane == c + 8, pltpu.roll(y_field, c + 8, 1), edges)
        turned_edges = jnp.concatenate([edges, jnp.zeros((Y - X, Y), F32)], axis=0).T
        y_out[phase, 0] = turned_edges[0:8, :]
        y_out[phase, 1] = turned_edges[8:16, :]

    def edges_of(phase):
        both = [y_in[phase, 0], y_in[phase, 1], jnp.zeros((Y - 16, Y), F32)]
        return jnp.concatenate(both, axis=0).T[:X, :]

    def halo_copies(phase):
        plan = (
            (x_out, x_in, 0, row < nrow - 1, row > 0, {"row": row + 1, "col": col}),
            (x_out, x_in, 1, row > 0, row < nrow - 1, {"row": row - 1, "col": col}),
            (y_out, y_in, 0, col < ncol - 1, col > 0, {"row": row, "col": col + 1}),
            (y_out, y_in, 1, col > 0, col < ncol - 1, {"row": row, "col": col - 1}),
        )
        copies = []
        for index, (source, target, way, sends, gets, device) in enumerate(plan):
            copy = pltpu.make_async_remote_copy(
                src_ref=source.at[phase, way],
                dst_ref=target.at[phase, way],
                send_sem=halo_send.at[phase, index],
                recv_sem=halo_recv.at[phase, index],
                device_id=device,
                device_id_type=MESH,
            )
            copies.append((copy, sends, gets))
        return copies

    def halo_start(phase):
        for copy, sends, _ in halo_copies(phase):
            pl.when(sends)(copy.start)

    def halo_wait(phase):
        for copy, sends, gets in halo_copies(phase):
            pl.when(gets)(copy.wait_recv)

    def halo_wait_sends(phase):
        for copy, sends, gets in halo_copies(phase):
            pl.when(sends)(copy.wait_send)

    def send(source, target, kind, device):
        pltpu.make_async_remote_copy(
            src_ref=source,
            dst_ref=target,
            send_sem=all_send.at[kind],
            recv_sem=all_recv.at[kind],
            device_id=device,
            device_id_type=MESH,
        ).start()

    def spread(source_of, target, kind, first, last):
        def one(k, carry):
            device, p = peer(k)
            send(source_of(p), target, kind, device)
            return carry

        lax.fori_loop(first, last, one, 0)

    def spread_wait(buffer, sem):
        pltpu.make_async_copy(buffer, buffer, sem).wait()

    direct_part = pl.ds(0, direct)
    shared_part = pl.ds(direct, pair - direct)

    def send_shared(out, inside, kind):
        if direct == pair:
            return

        def one(k, carry):
            p = side * half + lax.rem(lax.rem(here, half) + k, half)
            send(out.at[p, shared_part], inside.at[here, shared_part], kind, locate(p))
            return carry

        lax.fori_loop(1, half, one, 0)

    def send_direct(out, inside, kind, first, last):
        spread(
            lambda p: out.at[p, direct_part], inside.at[here, direct_part], kind, first, last
        )

    def forward(out, inside, kind):
        if direct == pair:
            return
        spread_wait(out.at[pl.ds(0, half - 1), shared_part], all_recv.at[kind])
        mine = inside.at[pl.ds(side * half, half), shared_part]
        send(mine, mine, kind + 2, locate(lax.rem(here + half, devices)))

    def rows_wait(inside, kind):
        spread_wait(inside.at[pl.ds(0, devices - 1), direct_part], all_recv.at[kind + 1])
        if direct < pair:
            spread_wait(inside.at[pl.ds(0, half), shared_part], all_recv.at[kind + 2])

    def sends_wait(inside, kind):
        spread_wait(inside.at[pl.ds(0, devices - 1), direct_part], all_send.at[kind + 1])
        if direct < pair:
            spread_wait(inside.at[pl.ds(0, half - 1), shared_part], all_send.at[kind])
            spread_wait(inside.at[pl.ds(0, half), shared_part], all_send.at[kind + 2])

    fetch[1].wait()
    fetch[2].wait()
    bond_x = 0.25 + 0.75 * bond_ref[0].astype(F32)
    bond_y = 0.25 + 0.75 * bond_ref[1].astype(F32)
    jump = [jump_ref[c] for c in range(3)]
    stage(0, [(jump[c], jump[c]) for c in range(3)] + [(bond_x, bond_y)])

    pl.semaphore_wait(barrier, devices - 1)

    count_in[pl.ds(here, 1)] = count_out[...][None]
    spread(lambda p: count_out, count_in.at[here], 0, 1, devices)
    halo_start(0)

    fetch[3].wait()
    slot_line = iota((slots, slots), 0)
    slot_lane = iota((slots, slots), 1)

    def to_column(values):
        return jnp.sum(jnp.where(slot_line == slot_lane, values, 0.0), axis=1, keepdims=True)

    points_row = points_ref[...]
    px_row = lax.shift_right_logical(points_row, (Y.bit_length() - 1))
    py_row = points_row & (Y - 1)
    px_col = to_column(px_row.astype(F32)).astype(jnp.int32)
    py_col = to_column(py_row.astype(F32)).astype(jnp.int32)
    steps_col = to_column(steps_row.astype(F32)).astype(jnp.int32)
    live_col = (steps_col > 0).astype(F32)
    at_x = (iota((slots, X), 1) == px_col).astype(F32).astype(BF16)
    at_y = (iota((slots, Y), 1) == py_col).astype(F32)
    at_x_turned = (iota((X, slots), 0) == px_row).astype(F32).astype(BF16)
    fetch[4].wait()
    drive = []
    for c in range(3):
        lines = picked(at_x, jump[c])
        drive.append(jnp.sum(lines * at_y, axis=1, keepdims=True))
    for start in range(0, cells, TILE):
        part = slice(start, start + TILE)
        total = drive[0] * coupling_ref[0:1, part]
        total = total + drive[1] * coupling_ref[1:2, part]
        load[:, part] = total + drive[2] * coupling_ref[2:3, part]
    rank_row = jnp.sum(jnp.where(slot_line < slot_lane, live_col, 0.0), axis=0, keepdims=True)

    fetch[5].wait()
    for start in range(0, cells, TILE):
        part = slice(start, start + TILE)
        damage[:, part] = jnp.exp(-history[:, part])
        for index, piece in enumerate(pieces_of(history[:, part])):
            pieces[index, :, part] = piece

    fetch[6].wait()
    fetch[7].wait()
    tile_eye = iota((TILE, TILE), 0) == iota((TILE, TILE), 1)
    for start in range(0, cells, TILE):
        part = slice(start, start + TILE)
        block = stiff[part, part].astype(F32)
        diagonal[:, part] = jnp.sum(jnp.where(tile_eye, block, 0.0), axis=0, keepdims=True)
        rounded[0, :, part] = state[:, part].astype(BF16)

    def advance(count, carry):
        now = lax.rem(count, 2)
        moves = count < steps_col
        for start in range(0, cells, TILE):
            part = slice(start, start + TILE)
            force = jnp.dot(rounded[now], stiff[:, part], preferred_element_type=F32)
            current = state[:, part]
            bent = jnp.tanh(current)
            worn = damage[:, part]
            misfit = force + worn * bent - load[:, part]
            slope = diagonal[:, part] + worn * (1.0 - bent * bent)
            current = jnp.where(moves, current - misfit / slope, current)
            state[:, part] = current
            rounded[1 - now, :, part] = current.astype(BF16)
        return carry

    lax.fori_loop(0, EARLY, advance, 0)

    spread_wait(count_in.at[pl.ds(0, devices - 1)], all_recv.at[0])
    counts = count_in[:, 0, :]
    device_line = iota((devices, LANES), 0)
    device_lane = iota((devices, LANES), 1)
    starts = jnp.sum(jnp.where(device_line < device_lane, counts, 0.0), axis=0, keepdims=True)
    ends = jnp.sum(jnp.where(device_line <= device_lane, counts, 0.0), axis=0, keepdims=True)
    my_start = jnp.sum(jnp.where(device_line < here, counts, 0.0), axis=0, keepdims=True)[:, :1]
    my_start = my_start.astype(jnp.int32)

    def place(rank, first):
        pairs = lax.shift_right_logical(rank, 1) - lax.shift_right_logical(first, 1)
        spot = 2 * lax.shift_right_logical(pairs, bits) + (rank & 1)
        if direct == pair:
            return spot
        spot = spot - jnp.where((pairs & (devices - 1)) == 0, first & 1, 0)
        return jnp.where(spot < direct, spot, direct + (rank & 1))

    ranks = rank_row.astype(jnp.int32) + my_start
    home = lax.shift_right_logical(ranks, 1) & (devices - 1)
    spots = place(ranks, my_start)
    if direct < pair:
        home = jnp.where(spots < direct, home, (home & (half - 1)) + side * half)
    leaves = jnp.where(steps_row > 0, home * padded + spots, -1)
    leaving = (iota((width, slots), 0) == leaves).astype(F32).astype(BF16)

    def gather_out(split_of, out):
        for start in range(0, cells, TILE):
            part = slice(start, start + TILE)
            rows = joined(leaving, split_of(part))
            out[:, :, part] = rows.reshape(devices, padded, TILE)

    gather_out(lambda part: [pieces[index, :, part] for index in range(3)], out_history)
    in_history[pl.ds(here, 1)] = out_history[pl.ds(here, 1)]
    send_shared(out_history, in_history, 1)
    send_direct(out_history, in_history, 2, 1, devices)

    wanted_slot = iota((new_cap, LANES), 0)
    wanted = 2 * (here + devices * lax.shift_right_logical(wanted_slot, 1)) + (wanted_slot & 1)
    wanted_lane = iota((new_cap, LANES), 1)
    wanted_float = wanted.astype(F32)
    hit = (starts <= wanted_float) & (wanted_float < ends) & (wanted_lane < devices)
    valid = jnp.sum(jnp.where(hit, 1.0, 0.0), axis=1, keepdims=True)
    from_start = jnp.sum(jnp.where(hit, starts, 0.0), axis=1, keepdims=True).astype(jnp.int32)
    source = jnp.sum(jnp.where(hit, wanted_lane.astype(F32), 0.0), axis=1, keepdims=True)
    arrives = source.astype(jnp.int32) * padded + place(wanted[:, :1], from_start)
    arrives = jnp.where(valid > 0.0, arrives, -1)
    coming = (iota((new_cap, width), 1) == arrives).astype(F32).astype(BF16)

    results = (
        (new_jump_ref, new_jump_hbm),
        (new_load_ref, new_load_hbm),
        (coming_ref, coming_hbm),
        (kept_ref, kept_hbm),
    )
    leave = []
    for index, (source, target) in enumerate(results):
        leave.append(pltpu.make_async_copy(source, target, result_sems.at[index]))
    coming_ref[...] = coming
    leave[2].start()

    lax.fori_loop(EARLY, MAX_STEPS, advance, 0)

    others = devices - 1
    bounds = [1] + [1 + others * s // 31 for s in CHUNKS] + [devices]

    gather_out(lambda part: pieces_of(state[:, part]), out_state)
    rows_part = pl.ds(0, pair)
    stays = pltpu.make_async_copy(
        out_state.at[here, rows_part], in_state.at[here, rows_part], result_sems.at[4]
    )
    stays.start()

    def send_state(step):
        if step == 0:
            send_shared(out_state, in_state, 4)
        send_direct(out_state, in_state, 5, bounds[step], bounds[step + 1])

    first_sum = jnp.zeros((slots, 16), F32)
    second_sum = jnp.zeros((slots, 16), F32)
    turned = (((1,), (1,)), ((), ()))

    def split(values):
        high = values.astype(BF16)
        return high, (values - high.astype(F32)).astype(BF16)

    def summed(values, factors):
        high, low = split(values)
        both = factors.astype(BF16).astype(F32)
        both = jnp.concatenate([both, factors - both], axis=0).astype(BF16)
        dot = functools.partial(
            lax.dot_general, dimension_numbers=turned, preferred_element_type=F32
        )
        return dot(high, both) + dot(low, both)

    for start in range(0, cells, TILE):
        part = slice(start, start + TILE)
        bent = jnp.tanh(state[:, part])
        worn = damage[:, part]
        a0, a1, a2 = [coupling_ref[a : a + 1, part] for a in range(3)]
        none = jnp.zeros((2, TILE), F32)
        firsts = jnp.concatenate([a0, a1, a2, none, none, none[:1]], axis=0)
        seconds = jnp.concatenate(
            [a0 * a0, a1 * a1, a2 * a2, a0 * a1, a0 * a2, a1 * a2, none], axis=0
        )
        first_sum = first_sum + summed(worn * bent, firsts)
        second_sum = second_sum + summed(worn * (1.0 - bent * bent), seconds)
    first_sum = (first_sum[:, :8] + first_sum[:, 8:]) * (live_col / cells)
    second_sum = (second_sum[:, :8] + second_sum[:, 8:]) * (live_col / cells)

    def put(values):
        return picked(at_x_turned, at_y * values)

    soft = put(live_col)
    rve_traction = [put(first_sum[:, c : c + 1]) for c in range(3)]
    tangent = [put(second_sum[:, c : c + 1]) for c in range(6)]

    halo_wait(0)
    for copy in fetch[8:]:
        copy.wait()

    def before_x(phase, field, c):
        return jnp.where(line == 0, x_in[phase, 0, c : c + 1, :], pltpu.roll(field, 1, 0))

    def after_x(phase, field, c):
        return jnp.where(line == X - 1, x_in[phase, 1, c : c + 1, :], pltpu.roll(field, X - 1, 0))

    def before_y(edges, field, c):
        edge = pltpu.roll(edges, (Y - c) % Y, 1)
        return jnp.where(lane == 0, edge, pltpu.roll(field, 1, 1))

    def after_y(edges, field, c):
        edge = pltpu.roll(edges, Y - 9 - c, 1)
        return jnp.where(lane == Y - 1, edge, pltpu.roll(field, Y - 1, 1))

    low_x = before_x(0, bond_x, 3)
    first_edges = edges_of(0)
    low_y = before_y(first_edges, bond_y, 3)

    def neighbours(phase, edges, field, c):
        return (
            bond_x * after_x(phase, field, c)
            + low_x * before_x(phase, field, c)
            + bond_y * after_y(edges, field, c)
            + low_y * before_y(edges, field, c)
        )

    scale = bond_x + low_x + bond_y + low_y + (1.0 - soft) * cohesive_ref[...]
    load_factor = load_ref[0]
    terms = []
    for c in range(3):
        residual = (
            scale * jump[c]
            - neighbours(0, first_edges, jump[c], c)
            + rve_traction[c]
            - load_factor * external_ref[c]
        )
        terms.append(-residual)
    for c in range(3):
        terms.append(external_ref[c])
    d00, d11, d22 = [scale + tangent[c] for c in range(3)]
    d01, d02, d12 = tangent[3:]
    c00 = d11 * d22 - d12 * d12
    c11 = d00 * d22 - d02 * d02
    c22 = d00 * d11 - d01 * d01
    c01 = d02 * d12 - d01 * d22
    c02 = d01 * d12 - d02 * d11
    c12 = d01 * d02 - d00 * d12
    inverse = 1.0 / (d00 * c00 + d01 * c01 + d02 * c02)
    c00, c11, c22, c01, c02, c12 = [c * inverse for c in (c00, c11, c22, c01, c02, c12)]

    def solve_both(w):
        result = []
        for h in (0, 3):
            result.append(c00 * w[h] + c01 * w[h + 1] + c02 * w[h + 2])
            result.append(c01 * w[h] + c11 * w[h + 1] + c12 * w[h + 2])
            result.append(c02 * w[h] + c12 * w[h + 1] + c22 * w[h + 2])
        return result

    iterate = solve_both(terms)
    peers = pl.ds(0, devices - 1)
    for sweep in range(SWEEPS):
        phase = sweep + 1
        stage(phase, [(v, v) for v in iterate])
        halo_start(phase)
        if sweep == 0:
            forward(out_history, in_history, 1)
        send_state(sweep)
        if sweep == 1:
            rows_wait(out_history, 1)
            for start in range(0, cells, TILE):
                part = slice(start, start + TILE)
                kept = picked(coming, in_history[:, :, part].reshape(width, TILE))
                kept_ref[:, part] = kept
            leave[3].start()
        if sweep == 2:
            stays.wait()
            forward(out_state, in_state, 4)
        halo_wait(phase)
        edges = edges_of(phase)
        iterate = solve_both([terms[c] + neighbours(phase, edges, iterate[c], c) for c in range(6)])
    correction, direction = iterate[:3], iterate[3:]

    def total_of(fields):
        return jnp.sum(fields[0] + fields[1] + fields[2], axis=0, keepdims=True)

    cross_row = total_of([correction[c] * direction[c] for c in range(3)])
    square_row = total_of([direction[c] * direction[c] for c in range(3)])
    own_cross = jnp.sum(cross_row, axis=1, keepdims=True)
    own_square = jnp.sum(square_row, axis=1, keepdims=True)
    sum_out[...] = jnp.where(iota((1, Y), 1) == 0, own_cross, own_square)
    sum_in[pl.ds(here, 1)] = sum_out[...][None]
    spread(lambda p: sum_out, sum_in.at[here], 7, 1, devices)
    send_state(SWEEPS)
    spread_wait(sum_in.at[pl.ds(0, devices - 1)], all_recv.at[7])
    sums = jnp.sum(sum_in[...], axis=0)
    cross = sums[:, 0:1]
    square = sums[:, 1:2]
    entries = 3.0 * X * Y * devices
    shifted = square + 0.25 * entries
    root = jnp.sqrt(shifted) * (entries**0.5)
    increment = (radius_ref[0] * root - cross) / shifted
    for c in range(3):
        new_jump_ref[c] = jump[c] + correction[c] + increment * direction[c]
    new_load_ref[...] = jnp.broadcast_to(load_factor + increment, new_load_ref.shape)
    leave[0].start()
    leave[1].start()

    rows_wait(out_state, 4)
    for copy in leave:
        copy.wait()
    for phase in range(SWEEPS + 1):
        halo_wait_sends(phase)
    spread_wait(count_in.at[peers], all_send.at[0])
    sends_wait(out_history, 1)
    sends_wait(out_state, 4)
    spread_wait(sum_in.at[peers], all_send.at[7])


def finish(
    pair,
    jump_hbm,
    load_hbm,
    coming_hbm,
    kept_hbm,
    rows_hbm,
    new_jump_hbm,
    new_load_ref,
    new_state_hbm,
    new_history_hbm,
    jump_ref,
    load_ref,
    coming_ref,
    kept_ref,
    rows_ref,
    state_ref,
    in_sems,
    row_sems,
    out_sems,
):
    devices, padded, cells = rows_ref.shape
    width = devices * padded
    parts = [pl.ds(start, WIDE) for start in range(0, cells, WIDE)]
    part_rows = pl.ds(0, pair)
    whole = pl.ds(0, devices)
    fetch = []
    names = (
        (coming_hbm, coming_ref),
        (jump_hbm, jump_ref),
        (load_hbm, load_ref),
        (kept_hbm, kept_ref),
    )
    for index, (source, target) in enumerate(names):
        fetch.append(pltpu.make_async_copy(source, target, in_sems.at[index]))
    fetch[0].start()
    rows = []
    for index, part in enumerate(parts):
        rows.append(
            pltpu.make_async_copy(
                rows_hbm.at[whole, part_rows, part],
                rows_ref.at[whole, part_rows, part],
                row_sems.at[index],
            )
        )
        rows[-1].start()
    for copy in fetch[1:]:
        copy.start()
    if pair < padded:
        rows_ref[:, pair:, :] = jnp.zeros((devices, padded - pair, cells), F32)
    stores = []

    def store(source, target):
        stores.append(pltpu.make_async_copy(source, target, out_sems.at[len(stores)]))
        stores[-1].start()

    fetch[0].wait()
    coming = coming_ref[...]
    for index, part in enumerate(parts):
        rows[index].wait()
        if index == 0:
            fetch[1].wait()
            store(jump_ref, new_jump_hbm)
            fetch[2].wait()
            new_load_ref[...] = load_ref[:, 0:1]
            fetch[3].wait()
        for start in range(index * WIDE, (index + 1) * WIDE, TILE):
            tile = slice(start, start + TILE)
            moved = picked(coming, rows_ref[:, :, tile].reshape(width, TILE))
            state_ref[:, tile] = moved
            kept_ref[:, tile] = jnp.maximum(kept_ref[:, tile], jnp.abs(moved))
        store(state_ref.at[:, part], new_state_hbm.at[:, part])
        store(kept_ref.at[:, part], new_history_hbm.at[:, part])
    for copy in stores:
        copy.wait()


def on_device(
    jump,
    external,
    cohesive,
    bond_mask,
    load_factor,
    arc_radius,
    stiffness,
    coupling,
    old_state,
    old_history,
    newton_steps,
    point_ids,
):
    nrow, ncol = lax.axis_size("row"), lax.axis_size("col")
    devices = nrow * ncol
    slots, cells = old_state.shape
    X, Y = cohesive.shape
    new_cap = slots // 2
    pair = 2 * ((slots + 2 * devices + 1) // (2 * devices))
    padded = 8 * ((pair + 7) // 8)
    phases = SWEEPS + 1
    shares = pair > 2 and nrow % 2 == 0 and slots <= (pair - 1) * devices
    direct = pair - 2 if shares else pair
    width = devices * padded
    landing = jax.ShapeDtypeStruct((devices, padded, cells), F32)
    between = (
        jax.ShapeDtypeStruct(jump.shape, F32),
        jax.ShapeDtypeStruct((1, LANES), F32),
        jax.ShapeDtypeStruct((new_cap, width), BF16),
        jax.ShapeDtypeStruct((new_cap, cells), F32),
        landing,
    )
    scratch = [pltpu.VMEM(shape.shape, shape.dtype) for shape in between]
    out_shape = (
        jax.ShapeDtypeStruct(jump.shape, F32),
        jax.ShapeDtypeStruct((1, 1), F32),
        jax.ShapeDtypeStruct((new_cap, cells), F32),
        jax.ShapeDtypeStruct((new_cap, cells), F32),
    )
    vmem = pl.BlockSpec(memory_space=pltpu.VMEM)
    hbm = pl.BlockSpec(memory_space=pltpu.HBM)
    results = pl.pallas_call(
        functools.partial(body, nrow, ncol, pair, direct),
        out_shape=between,
        in_specs=[hbm] * 12,
        out_specs=(hbm,) * 5,
        scratch_shapes=scratch[:4]
        + [
            pltpu.VMEM((3, slots, cells), BF16),
            pltpu.VMEM(jump.shape, F32),
            pltpu.VMEM(external.shape, F32),
            pltpu.VMEM(cohesive.shape, F32),
            pltpu.VMEM(bond_mask.shape, jnp.int32),
            pltpu.SMEM((1,), F32),
            pltpu.SMEM((1,), F32),
            pltpu.VMEM(coupling.shape, F32),
            pltpu.VMEM((1, slots), jnp.int32),
            pltpu.VMEM((1, slots), jnp.int32),
            pltpu.VMEM((cells, cells), BF16),
            pltpu.VMEM((slots, cells), F32),
            pltpu.VMEM((slots, cells), F32),
            pltpu.VMEM((slots, cells), F32),
            pltpu.VMEM((slots, cells), F32),
            pltpu.VMEM((2, slots, cells), BF16),
            pltpu.VMEM((1, cells), F32),
            pltpu.VMEM((1, LANES), F32),
            pltpu.VMEM((devices, 1, LANES), F32),
            pltpu.VMEM((1, Y), F32),
            pltpu.VMEM((devices, 1, Y), F32),
            pltpu.VMEM((phases, 2, 8, Y), F32),
            pltpu.VMEM((phases, 2, 8, Y), F32),
            pltpu.VMEM((phases, 2, 8, Y), F32),
            pltpu.VMEM((phases, 2, 8, Y), F32),
            pltpu.VMEM((devices, padded, cells), F32),
            pltpu.VMEM((devices, padded, cells), F32),
            pltpu.VMEM((devices, padded, cells), F32),
            pltpu.SemaphoreType.DMA((12,)),
            pltpu.SemaphoreType.DMA((5,)),
            pltpu.SemaphoreType.DMA((phases, 4)),
            pltpu.SemaphoreType.DMA((phases, 4)),
            pltpu.SemaphoreType.DMA((8,)),
            pltpu.SemaphoreType.DMA((8,)),
        ],
        compiler_params=pltpu.CompilerParams(
            collective_id=0, has_side_effects=True, vmem_limit_bytes=GRANT
        ),
    )(
        jump,
        external,
        cohesive,
        bond_mask,
        load_factor,
        arc_radius,
        coupling,
        newton_steps.reshape(1, slots),
        point_ids.reshape(1, slots),
        stiffness,
        old_state,
        old_history,
    )
    new_jump, new_load, new_state, new_history = pl.pallas_call(
        functools.partial(finish, pair),
        out_shape=out_shape,
        in_specs=[hbm] * 5,
        out_specs=(hbm, vmem, hbm, hbm),
        scratch_shapes=scratch
        + [
            pltpu.VMEM((new_cap, cells), F32),
            pltpu.SemaphoreType.DMA((4,)),
            pltpu.SemaphoreType.DMA((cells // WIDE,)),
            pltpu.SemaphoreType.DMA((2 * (cells // WIDE) + 1,)),
        ],
        compiler_params=pltpu.CompilerParams(vmem_limit_bytes=GRANT),
    )(*results)
    return new_jump, new_load.reshape(1), new_state, new_history


def solution(mesh):
    in_specs = (
        P(None, "row", "col"),
        P(None, "row", "col"),
        P("row", "col"),
        P(None, "row", "col"),
        P(),
        P(),
        P(),
        P(),
        P(("row", "col"), None),
        P(("row", "col"), None),
        P(("row", "col")),
        P(("row", "col")),
    )
    out_specs = (P(None, "row", "col"), P(), P(("row", "col"), None), P(("row", "col"), None))
    return jax.shard_map(
        on_device, mesh=mesh, in_specs=in_specs, out_specs=out_specs, check_vma=False
    )
```

```python
import functools

import jax
import jax.numpy as jnp
from jax import lax
from jax.experimental import pallas as pl
from jax.experimental.pallas import tpu as pltpu
from jax.sharding import PartitionSpec as P

MAX_STEPS = 9
SWEEPS = 3
TILE = 256
WIDE = 768
EARLY = 1
GRANT = 60 * 1024 * 1024
CHUNKS = (4, 11, 19)
LANES = 128
MESH = pl.DeviceIdType.MESH
F32 = jnp.float32
BF16 = jnp.bfloat16


def iota(shape, dim):
    return lax.broadcasted_iota(jnp.int32, shape, dim)


def pieces_of(values):
    high = values.astype(BF16)
    rest = values - high.astype(F32)
    middle = rest.astype(BF16)
    low = (rest - middle.astype(F32)).astype(BF16)
    return high, middle, low


def joined(onehot, pieces):
    dot = functools.partial(jnp.dot, preferred_element_type=F32)
    return dot(onehot, pieces[0]) + dot(onehot, pieces[1]) + dot(onehot, pieces[2])


def picked(onehot, values):
    return joined(onehot, pieces_of(values))


def body(
    nrow,
    ncol,
    pair,
    direct,
    jump_hbm,
    external_hbm,
    cohesive_hbm,
    bond_hbm,
    load_hbm,
    radius_hbm,
    coupling_hbm,
    steps_hbm,
    points_hbm,
    stiffness_hbm,
    state_hbm,
    history_hbm,
    new_jump_hbm,
    new_load_hbm,
    coming_hbm,
    kept_hbm,
    in_state,
    new_jump_ref,
    new_load_ref,
    coming_ref,
    kept_ref,
    pieces,
    jump_ref,
    external_ref,
    cohesive_ref,
    bond_ref,
    load_ref,
    radius_ref,
    coupling_ref,
    steps_ref,
    points_ref,
    stiff,
    state,
    history,
    damage,
    load,
    rounded,
    diagonal,
    count_out,
    count_in,
    sum_out,
    sum_in,
    x_out,
    x_in,
    y_out,
    y_in,
    out_history,
    in_history,
    out_state,
    local_sems,
    result_sems,
    halo_send,
    halo_recv,
    all_send,
    all_recv,
):
    devices = nrow * ncol
    row, col = lax.axis_index("row"), lax.axis_index("col")
    here = row * ncol + col
    slots, cells = state.shape
    X, Y = cohesive_ref.shape
    new_cap = kept_ref.shape[0]
    padded = out_history.shape[1]
    width = devices * padded
    bits = devices.bit_length() - 1

    half = devices // 2
    side = lax.div(row, nrow // 2)

    names = (
        (steps_hbm, steps_ref),
        (jump_hbm, jump_ref),
        (bond_hbm, bond_ref),
        (points_hbm, points_ref),
        (coupling_hbm, coupling_ref),
        (history_hbm, history),
        (stiffness_hbm, stiff),
        (state_hbm, state),
        (external_hbm, external_ref),
        (cohesive_hbm, cohesive_ref),
        (load_hbm, load_ref),
        (radius_hbm, radius_ref),
    )
    fetch = []
    for index, (source, target) in enumerate(names):
        fetch.append(pltpu.make_async_copy(source, target, local_sems.at[index]))
    fetch[0].start()

    def locate(p):
        return {"row": lax.div(p, ncol), "col": lax.rem(p, ncol)}

    def peer(k):
        p = lax.rem(here + k, devices)
        return locate(p), p

    x_in[...] = jnp.zeros_like(x_in)
    y_in[...] = jnp.zeros_like(y_in)

    barrier = pltpu.get_barrier_semaphore()

    def greet(k, carry):
        device, _ = peer(k)
        pl.semaphore_signal(barrier, inc=1, device_id=device, device_id_type=MESH)
        return carry

    lax.fori_loop(1, devices, greet, 0)
    for copy in fetch[1:]:
        copy.start()

    if pair < padded:
        blank = jnp.zeros((devices, padded - pair, cells), F32)
        in_history[:, pair:, :] = blank

    fetch[0].wait()
    steps_row = steps_ref[...]
    live_row = (steps_row > 0).astype(F32)
    count_out[...] = jnp.broadcast_to(jnp.sum(live_row, axis=1, keepdims=True), count_out.shape)

    lane = iota((X, Y), 1)
    line = iota((X, Y), 0)

    def stage(phase, fields):
        edges = jnp.zeros((X, Y), F32)
        for c, (x_field, y_field) in enumerate(fields):
            x_out[phase, 0, c : c + 1, :] = x_field[X - 1 : X, :]
            x_out[phase, 1, c : c + 1, :] = x_field[0:1, :]
            edges = jnp.where(lane == c, pltpu.roll(y_field, (c + 1) % Y, 1), edges)
            edges = jnp.where(lane == c + 8, pltpu.roll(y_field, c + 8, 1), edges)
        turned_edges = jnp.concatenate([edges, jnp.zeros((Y - X, Y), F32)], axis=0).T
        y_out[phase, 0] = turned_edges[0:8, :]
        y_out[phase, 1] = turned_edges[8:16, :]

    def edges_of(phase):
        both = [y_in[phase, 0], y_in[phase, 1], jnp.zeros((Y - 16, Y), F32)]
        return jnp.concatenate(both, axis=0).T[:X, :]

    def halo_copies(phase):
        plan = (
            (x_out, x_in, 0, row < nrow - 1, row > 0, {"row": row + 1, "col": col}),
            (x_out, x_in, 1, row > 0, row < nrow - 1, {"row": row - 1, "col": col}),
            (y_out, y_in, 0, col < ncol - 1, col > 0, {"row": row, "col": col + 1}),
            (y_out, y_in, 1, col > 0, col < ncol - 1, {"row": row, "col": col - 1}),
        )
        copies = []
        for index, (source, target, way, sends, gets, device) in enumerate(plan):
            copy = pltpu.make_async_remote_copy(
                src_ref=source.at[phase, way],
                dst_ref=target.at[phase, way],
                send_sem=halo_send.at[phase, index],
                recv_sem=halo_recv.at[phase, index],
                device_id=device,
                device_id_type=MESH,
            )
            copies.append((copy, sends, gets))
        return copies

    def halo_start(phase):
        for copy, sends, _ in halo_copies(phase):
            pl.when(sends)(copy.start)

    def halo_wait(phase):
        for copy, sends, gets in halo_copies(phase):
            pl.when(gets)(copy.wait_recv)

    def halo_wait_sends(phase):
        for copy, sends, gets in halo_copies(phase):
            pl.when(sends)(copy.wait_send)

    def send(source, target, kind, device):
        pltpu.make_async_remote_copy(
            src_ref=source,
            dst_ref=target,
            send_sem=all_send.at[kind],
            recv_sem=all_recv.at[kind],
            device_id=device,
            device_id_type=MESH,
        ).start()

    def spread(source_of, target, kind, first, last):
        def one(k, carry):
            device, p = peer(k)
            send(source_of(p), target, kind, device)
            return carry

        lax.fori_loop(first, last, one, 0)

    def spread_wait(buffer, sem):
        pltpu.make_async_copy(buffer, buffer, sem).wait()

    direct_part = pl.ds(0, direct)
    shared_part = pl.ds(direct, pair - direct)

    def send_shared(out, inside, kind):
        if direct == pair:
            return

        def one(k, carry):
            p = side * half + lax.rem(lax.rem(here, half) + k, half)
            send(out.at[p, shared_part], inside.at[here, shared_part], kind, locate(p))
            return carry

        lax.fori_loop(1, half, one, 0)

    def send_direct(out, inside, kind, first, last):
        spread(
            lambda p: out.at[p, direct_part], inside.at[here, direct_part], kind, first, last
        )

    def forward(out, inside, kind):
        if direct == pair:
            return
        spread_wait(out.at[pl.ds(0, half - 1), shared_part], all_recv.at[kind])
        mine = inside.at[pl.ds(side * half, half), shared_part]
        send(mine, mine, kind + 2, locate(lax.rem(here + half, devices)))

    def rows_wait(inside, kind):
        spread_wait(inside.at[pl.ds(0, devices - 1), direct_part], all_recv.at[kind + 1])
        if direct < pair:
            spread_wait(inside.at[pl.ds(0, half), shared_part], all_recv.at[kind + 2])

    def sends_wait(inside, kind):
        spread_wait(inside.at[pl.ds(0, devices - 1), direct_part], all_send.at[kind + 1])
        if direct < pair:
            spread_wait(inside.at[pl.ds(0, half - 1), shared_part], all_send.at[kind])
            spread_wait(inside.at[pl.ds(0, half), shared_part], all_send.at[kind + 2])

    fetch[1].wait()
    fetch[2].wait()
    bond_x = 0.25 + 0.75 * bond_ref[0].astype(F32)
    bond_y = 0.25 + 0.75 * bond_ref[1].astype(F32)
    jump = [jump_ref[c] for c in range(3)]
    stage(0, [(jump[c], jump[c]) for c in range(3)] + [(bond_x, bond_y)])

    pl.semaphore_wait(barrier, devices - 1)

    count_in[pl.ds(here, 1)] = count_out[...][None]
    spread(lambda p: count_out, count_in.at[here], 0, 1, devices)
    halo_start(0)

    fetch[3].wait()
    slot_line = iota((slots, slots), 0)
    slot_lane = iota((slots, slots), 1)

    def to_column(values):
        return jnp.sum(jnp.where(slot_line == slot_lane, values, 0.0), axis=1, keepdims=True)

    points_row = points_ref[...]
    px_row = lax.shift_right_logical(points_row, (Y.bit_length() - 1))
    py_row = points_row & (Y - 1)
    px_col = to_column(px_row.astype(F32)).astype(jnp.int32)
    py_col = to_column(py_row.astype(F32)).astype(jnp.int32)
    steps_col = to_column(steps_row.astype(F32)).astype(jnp.int32)
    live_col = (steps_col > 0).astype(F32)
    at_x = (iota((slots, X), 1) == px_col).astype(F32).astype(BF16)
    at_y = (iota((slots, Y), 1) == py_col).astype(F32)
    at_x_turned = (iota((X, slots), 0) == px_row).astype(F32).astype(BF16)
    fetch[4].wait()
    drive = []
    for c in range(3):
        lines = picked(at_x, jump[c])
        drive.append(jnp.sum(lines * at_y, axis=1, keepdims=True))
    for start in range(0, cells, TILE):
        part = slice(start, start + TILE)
        total = drive[0] * coupling_ref[0:1, part]
        total = total + drive[1] * coupling_ref[1:2, part]
        load[:, part] = total + drive[2] * coupling_ref[2:3, part]
    rank_row = jnp.sum(jnp.where(slot_line < slot_lane, live_col, 0.0), axis=0, keepdims=True)

    fetch[5].wait()
    for start in range(0, cells, TILE):
        part = slice(start, start + TILE)
        damage[:, part] = jnp.exp(-history[:, part])
        for index, piece in enumerate(pieces_of(history[:, part])):
            pieces[index, :, part] = piece

    fetch[6].wait()
    fetch[7].wait()
    tile_eye = iota((TILE, TILE), 0) == iota((TILE, TILE), 1)
    for start in range(0, cells, TILE):
        part = slice(start, start + TILE)
        block = stiff[part, part].astype(F32)
        diagonal[:, part] = jnp.sum(jnp.where(tile_eye, block, 0.0), axis=0, keepdims=True)
        rounded[0, :, part] = state[:, part].astype(BF16)

    def advance(count, carry):
        now = lax.rem(count, 2)
        moves = count < steps_col
        for start in range(0, cells, TILE):
            part = slice(start, start + TILE)
            force = jnp.dot(rounded[now], stiff[:, part], preferred_element_type=F32)
            current = state[:, part]
            bent = jnp.tanh(current)
            worn = damage[:, part]
            misfit = force + worn * bent - load[:, part]
            slope = diagonal[:, part] + worn * (1.0 - bent * bent)
            current = jnp.where(moves, current - misfit / slope, current)
            state[:, part] = current
            rounded[1 - now, :, part] = current.astype(BF16)
        return carry

    lax.fori_loop(0, EARLY, advance, 0)

    spread_wait(count_in.at[pl.ds(0, devices - 1)], all_recv.at[0])
    counts = count_in[:, 0, :]
    device_line = iota((devices, LANES), 0)
    device_lane = iota((devices, LANES), 1)
    starts = jnp.sum(jnp.where(device_line < device_lane, counts, 0.0), axis=0, keepdims=True)
    ends = jnp.sum(jnp.where(device_line <= device_lane, counts, 0.0), axis=0, keepdims=True)
    my_start = jnp.sum(jnp.where(device_line < here, counts, 0.0), axis=0, keepdims=True)[:, :1]
    my_start = my_start.astype(jnp.int32)

    def place(rank, first):
        pairs = lax.shift_right_logical(rank, 1) - lax.shift_right_logical(first, 1)
        spot = 2 * lax.shift_right_logical(pairs, bits) + (rank & 1)
        if direct == pair:
            return spot
        spot = spot - jnp.where((pairs & (devices - 1)) == 0, first & 1, 0)
        return jnp.where(spot < direct, spot, direct + (rank & 1))

    ranks = rank_row.astype(jnp.int32) + my_start
    home = lax.shift_right_logical(ranks, 1) & (devices - 1)
    spots = place(ranks, my_start)
    if direct < pair:
        home = jnp.where(spots < direct, home, (home & (half - 1)) + side * half)
    leaves = jnp.where(steps_row > 0, home * padded + spots, -1)
    leaving = (iota((width, slots), 0) == leaves).astype(F32).astype(BF16)

    def gather_out(split_of, out):
        for start in range(0, cells, TILE):
            part = slice(start, start + TILE)
            rows = joined(leaving, split_of(part))
            out[:, :, part] = rows.reshape(devices, padded, TILE)

    gather_out(lambda part: [pieces[index, :, part] for index in range(3)], out_history)
    in_history[pl.ds(here, 1)] = out_history[pl.ds(here, 1)]
    send_shared(out_history, in_history, 1)
    send_direct(out_history, in_history, 2, 1, devices)

    wanted_slot = iota((new_cap, LANES), 0)
    wanted = 2 * (here + devices * lax.shift_right_logical(wanted_slot, 1)) + (wanted_slot & 1)
    wanted_lane = iota((new_cap, LANES), 1)
    wanted_float = wanted.astype(F32)
    hit = (starts <= wanted_float) & (wanted_float < ends) & (wanted_lane < devices)
    valid = jnp.sum(jnp.where(hit, 1.0, 0.0), axis=1, keepdims=True)
    from_start = jnp.sum(jnp.where(hit, starts, 0.0), axis=1, keepdims=True).astype(jnp.int32)
    source = jnp.sum(jnp.where(hit, wanted_lane.astype(F32), 0.0), axis=1, keepdims=True)
    arrives = source.astype(jnp.int32) * padded + place(wanted[:, :1], from_start)
    arrives = jnp.where(valid > 0.0, arrives, -1)
    coming = (iota((new_cap, width), 1) == arrives).astype(F32).astype(BF16)

    results = (
        (new_jump_ref, new_jump_hbm),
        (new_load_ref, new_load_hbm),
        (coming_ref, coming_hbm),
        (kept_ref, kept_hbm),
    )
    leave = []
    for index, (source, target) in enumerate(results):
        leave.append(pltpu.make_async_copy(source, target, result_sems.at[index]))
    coming_ref[...] = coming
    leave[2].start()

    lax.fori_loop(EARLY, MAX_STEPS, advance, 0)

    others = devices - 1
    bounds = [1] + [1 + others * s // 31 for s in CHUNKS] + [devices]

    gather_out(lambda part: pieces_of(state[:, part]), out_state)
    rows_part = pl.ds(0, pair)
    stays = pltpu.make_async_copy(
        out_state.at[here, rows_part], in_state.at[here, rows_part], result_sems.at[4]
    )
    stays.start()

    def send_state(step):
        if step == 0:
            send_shared(out_state, in_state, 4)
        send_direct(out_state, in_state, 5, bounds[step], bounds[step + 1])

    first_sum = jnp.zeros((slots, 16), F32)
    second_sum = jnp.zeros((slots, 16), F32)
    turned = (((1,), (1,)), ((), ()))

    def split(values):
        high = values.astype(BF16)
        return high, (values - high.astype(F32)).astype(BF16)

    def summed(values, factors):
        high, low = split(values)
        both = factors.astype(BF16).astype(F32)
        both = jnp.concatenate([both, factors - both], axis=0).astype(BF16)
        dot = functools.partial(
            lax.dot_general, dimension_numbers=turned, preferred_element_type=F32
        )
        return dot(high, both) + dot(low, both)

    for start in range(0, cells, TILE):
        part = slice(start, start + TILE)
        bent = jnp.tanh(state[:, part])
        worn = damage[:, part]
        a0, a1, a2 = [coupling_ref[a : a + 1, part] for a in range(3)]
        none = jnp.zeros((2, TILE), F32)
        firsts = jnp.concatenate([a0, a1, a2, none, none, none[:1]], axis=0)
        seconds = jnp.concatenate(
            [a0 * a0, a1 * a1, a2 * a2, a0 * a1, a0 * a2, a1 * a2, none], axis=0
        )
        first_sum = first_sum + summed(worn * bent, firsts)
        second_sum = second_sum + summed(worn * (1.0 - bent * bent), seconds)
    first_sum = (first_sum[:, :8] + first_sum[:, 8:]) * (live_col / cells)
    second_sum = (second_sum[:, :8] + second_sum[:, 8:]) * (live_col / cells)

    def put(values):
        return picked(at_x_turned, at_y * values)

    soft = put(live_col)
    rve_traction = [put(first_sum[:, c : c + 1]) for c in range(3)]
    tangent = [put(second_sum[:, c : c + 1]) for c in range(6)]

    halo_wait(0)
    for copy in fetch[8:]:
        copy.wait()

    def before_x(phase, field, c):
        return jnp.where(line == 0, x_in[phase, 0, c : c + 1, :], pltpu.roll(field, 1, 0))

    def after_x(phase, field, c):
        return jnp.where(line == X - 1, x_in[phase, 1, c : c + 1, :], pltpu.roll(field, X - 1, 0))

    def before_y(edges, field, c):
        edge = pltpu.roll(edges, (Y - c) % Y, 1)
        return jnp.where(lane == 0, edge, pltpu.roll(field, 1, 1))

    def after_y(edges, field, c):
        edge = pltpu.roll(edges, Y - 9 - c, 1)
        return jnp.where(lane == Y - 1, edge, pltpu.roll(field, Y - 1, 1))

    low_x = before_x(0, bond_x, 3)
    first_edges = edges_of(0)
    low_y = before_y(first_edges, bond_y, 3)

    def neighbours(phase, edges, field, c):
        return (
            bond_x * after_x(phase, field, c)
            + low_x * before_x(phase, field, c)
            + bond_y * after_y(edges, field, c)
            + low_y * before_y(edges, field, c)
        )

    scale = bond_x + low_x + bond_y + low_y + (1.0 - soft) * cohesive_ref[...]
    load_factor = load_ref[0]
    terms = []
    for c in range(3):
        residual = (
            scale * jump[c]
            - neighbours(0, first_edges, jump[c], c)
            + rve_traction[c]
            - load_factor * external_ref[c]
        )
        terms.append(-residual)
    for c in range(3):
        terms.append(external_ref[c])
    d00, d11, d22 = [scale + tangent[c] for c in range(3)]
    d01, d02, d12 = tangent[3:]
    c00 = d11 * d22 - d12 * d12
    c11 = d00 * d22 - d02 * d02
    c22 = d00 * d11 - d01 * d01
    c01 = d02 * d12 - d01 * d22
    c02 = d01 * d12 - d02 * d11
    c12 = d01 * d02 - d00 * d12
    inverse = 1.0 / (d00 * c00 + d01 * c01 + d02 * c02)
    c00, c11, c22, c01, c02, c12 = [c * inverse for c in (c00, c11, c22, c01, c02, c12)]

    def solve_both(w):
        result = []
        for h in (0, 3):
            result.append(c00 * w[h] + c01 * w[h + 1] + c02 * w[h + 2])
            result.append(c01 * w[h] + c11 * w[h + 1] + c12 * w[h + 2])
            result.append(c02 * w[h] + c12 * w[h + 1] + c22 * w[h + 2])
        return result

    iterate = solve_both(terms)
    peers = pl.ds(0, devices - 1)
    for sweep in range(SWEEPS):
        phase = sweep + 1
        stage(phase, [(v, v) for v in iterate])
        halo_start(phase)
        send_state(sweep)
        if sweep == 0:
            forward(out_history, in_history, 1)
        if sweep == 1:
            rows_wait(out_history, 1)
            for start in range(0, cells, TILE):
                part = slice(start, start + TILE)
                kept = picked(coming, in_history[:, :, part].reshape(width, TILE))
                kept_ref[:, part] = kept
            leave[3].start()
        if sweep == 2:
            stays.wait()
            forward(out_state, in_state, 4)
        halo_wait(phase)
        edges = edges_of(phase)
        iterate = solve_both([terms[c] + neighbours(phase, edges, iterate[c], c) for c in range(6)])
    correction, direction = iterate[:3], iterate[3:]

    def total_of(fields):
        return jnp.sum(fields[0] + fields[1] + fields[2], axis=0, keepdims=True)

    cross_row = total_of([correction[c] * direction[c] for c in range(3)])
    square_row = total_of([direction[c] * direction[c] for c in range(3)])
    own_cross = jnp.sum(cross_row, axis=1, keepdims=True)
    own_square = jnp.sum(square_row, axis=1, keepdims=True)
    sum_out[...] = jnp.where(iota((1, Y), 1) == 0, own_cross, own_square)
    sum_in[pl.ds(here, 1)] = sum_out[...][None]
    spread(lambda p: sum_out, sum_in.at[here], 7, 1, devices)
    send_state(SWEEPS)
    spread_wait(sum_in.at[pl.ds(0, devices - 1)], all_recv.at[7])
    sums = jnp.sum(sum_in[...], axis=0)
    cross = sums[:, 0:1]
    square = sums[:, 1:2]
    entries = 3.0 * X * Y * devices
    shifted = square + 0.25 * entries
    root = jnp.sqrt(shifted) * (entries**0.5)
    increment = (radius_ref[0] * root - cross) / shifted
    for c in range(3):
        new_jump_ref[c] = jump[c] + correction[c] + increment * direction[c]
    new_load_ref[...] = jnp.broadcast_to(load_factor + increment, new_load_ref.shape)
    leave[0].start()
    leave[1].start()

    rows_wait(out_state, 4)
    for copy in leave:
        copy.wait()
    for phase in range(SWEEPS + 1):
        halo_wait_sends(phase)
    spread_wait(count_in.at[peers], all_send.at[0])
    sends_wait(out_history, 1)
    sends_wait(out_state, 4)
    spread_wait(sum_in.at[peers], all_send.at[7])


def finish(
    pair,
    jump_hbm,
    load_hbm,
    coming_hbm,
    kept_hbm,
    rows_hbm,
    new_jump_hbm,
    new_load_ref,
    new_state_hbm,
    new_history_hbm,
    jump_ref,
    load_ref,
    coming_ref,
    kept_ref,
    rows_ref,
    state_ref,
    in_sems,
    row_sems,
    out_sems,
):
    devices, padded, cells = rows_ref.shape
    width = devices * padded
    parts = [pl.ds(start, WIDE) for start in range(0, cells, WIDE)]
    part_rows = pl.ds(0, pair)
    whole = pl.ds(0, devices)
    fetch = []
    names = (
        (coming_hbm, coming_ref),
        (jump_hbm, jump_ref),
        (load_hbm, load_ref),
        (kept_hbm, kept_ref),
    )
    for index, (source, target) in enumerate(names):
        fetch.append(pltpu.make_async_copy(source, target, in_sems.at[index]))
    fetch[0].start()
    rows = []
    for index, part in enumerate(parts):
        rows.append(
            pltpu.make_async_copy(
                rows_hbm.at[whole, part_rows, part],
                rows_ref.at[whole, part_rows, part],
                row_sems.at[index],
            )
        )
        rows[-1].start()
    for copy in fetch[1:]:
        copy.start()
    if pair < padded:
        rows_ref[:, pair:, :] = jnp.zeros((devices, padded - pair, cells), F32)
    stores = []

    def store(source, target):
        stores.append(pltpu.make_async_copy(source, target, out_sems.at[len(stores)]))
        stores[-1].start()

    fetch[0].wait()
    coming = coming_ref[...]
    for index, part in enumerate(parts):
        rows[index].wait()
        if index == 0:
            fetch[1].wait()
            store(jump_ref, new_jump_hbm)
            fetch[2].wait()
            new_load_ref[...] = load_ref[:, 0:1]
            fetch[3].wait()
        for start in range(index * WIDE, (index + 1) * WIDE, TILE):
            tile = slice(start, start + TILE)
            moved = picked(coming, rows_ref[:, :, tile].reshape(width, TILE))
            state_ref[:, tile] = moved
            kept_ref[:, tile] = jnp.maximum(kept_ref[:, tile], jnp.abs(moved))
        store(state_ref.at[:, part], new_state_hbm.at[:, part])
        store(kept_ref.at[:, part], new_history_hbm.at[:, part])
    for copy in stores:
        copy.wait()


def on_device(
    jump,
    external,
    cohesive,
    bond_mask,
    load_factor,
    arc_radius,
    stiffness,
    coupling,
    old_state,
    old_history,
    newton_steps,
    point_ids,
):
    nrow, ncol = lax.axis_size("row"), lax.axis_size("col")
    devices = nrow * ncol
    slots, cells = old_state.shape
    X, Y = cohesive.shape
    new_cap = slots // 2
    pair = 2 * ((slots + 2 * devices + 1) // (2 * devices))
    padded = 8 * ((pair + 7) // 8)
    phases = SWEEPS + 1
    shares = pair > 2 and nrow % 2 == 0 and slots <= (pair - 1) * devices
    direct = pair - 2 if shares else pair
    width = devices * padded
    landing = jax.ShapeDtypeStruct((devices, padded, cells), F32)
    between = (
        jax.ShapeDtypeStruct(jump.shape, F32),
        jax.ShapeDtypeStruct((1, LANES), F32),
        jax.ShapeDtypeStruct((new_cap, width), BF16),
        jax.ShapeDtypeStruct((new_cap, cells), F32),
        landing,
    )
    scratch = [pltpu.VMEM(shape.shape, shape.dtype) for shape in between]
    out_shape = (
        jax.ShapeDtypeStruct(jump.shape, F32),
        jax.ShapeDtypeStruct((1, 1), F32),
        jax.ShapeDtypeStruct((new_cap, cells), F32),
        jax.ShapeDtypeStruct((new_cap, cells), F32),
    )
    vmem = pl.BlockSpec(memory_space=pltpu.VMEM)
    hbm = pl.BlockSpec(memory_space=pltpu.HBM)
    results = pl.pallas_call(
        functools.partial(body, nrow, ncol, pair, direct),
        out_shape=between,
        in_specs=[hbm] * 12,
        out_specs=(hbm,) * 5,
        scratch_shapes=scratch[:4]
        + [
            pltpu.VMEM((3, slots, cells), BF16),
            pltpu.VMEM(jump.shape, F32),
            pltpu.VMEM(external.shape, F32),
            pltpu.VMEM(cohesive.shape, F32),
            pltpu.VMEM(bond_mask.shape, jnp.int32),
            pltpu.SMEM((1,), F32),
            pltpu.SMEM((1,), F32),
            pltpu.VMEM(coupling.shape, F32),
            pltpu.VMEM((1, slots), jnp.int32),
            pltpu.VMEM((1, slots), jnp.int32),
            pltpu.VMEM((cells, cells), BF16),
            pltpu.VMEM((slots, cells), F32),
            pltpu.VMEM((slots, cells), F32),
            pltpu.VMEM((slots, cells), F32),
            pltpu.VMEM((slots, cells), F32),
            pltpu.VMEM((2, slots, cells), BF16),
            pltpu.VMEM((1, cells), F32),
            pltpu.VMEM((1, LANES), F32),
            pltpu.VMEM((devices, 1, LANES), F32),
            pltpu.VMEM((1, Y), F32),
            pltpu.VMEM((devices, 1, Y), F32),
            pltpu.VMEM((phases, 2, 8, Y), F32),
            pltpu.VMEM((phases, 2, 8, Y), F32),
            pltpu.VMEM((phases, 2, 8, Y), F32),
            pltpu.VMEM((phases, 2, 8, Y), F32),
            pltpu.VMEM((devices, padded, cells), F32),
            pltpu.VMEM((devices, padded, cells), F32),
            pltpu.VMEM((devices, padded, cells), F32),
            pltpu.SemaphoreType.DMA((12,)),
            pltpu.SemaphoreType.DMA((5,)),
            pltpu.SemaphoreType.DMA((phases, 4)),
            pltpu.SemaphoreType.DMA((phases, 4)),
            pltpu.SemaphoreType.DMA((8,)),
            pltpu.SemaphoreType.DMA((8,)),
        ],
        compiler_params=pltpu.CompilerParams(
            collective_id=0, has_side_effects=True, vmem_limit_bytes=GRANT
        ),
    )(
        jump,
        external,
        cohesive,
        bond_mask,
        load_factor,
        arc_radius,
        coupling,
        newton_steps.reshape(1, slots),
        point_ids.reshape(1, slots),
        stiffness,
        old_state,
        old_history,
    )
    new_jump, new_load, new_state, new_history = pl.pallas_call(
        functools.partial(finish, pair),
        out_shape=out_shape,
        in_specs=[hbm] * 5,
        out_specs=(hbm, vmem, hbm, hbm),
        scratch_shapes=scratch
        + [
            pltpu.VMEM((new_cap, cells), F32),
            pltpu.SemaphoreType.DMA((4,)),
            pltpu.SemaphoreType.DMA((cells // WIDE,)),
            pltpu.SemaphoreType.DMA((2 * (cells // WIDE) + 1,)),
        ],
        compiler_params=pltpu.CompilerParams(vmem_limit_bytes=GRANT),
    )(*results)
    return new_jump, new_load.reshape(1), new_state, new_history


def solution(mesh):
    in_specs = (
        P(None, "row", "col"),
        P(None, "row", "col"),
        P("row", "col"),
        P(None, "row", "col"),
        P(),
        P(),
        P(),
        P(),
        P(("row", "col"), None),
        P(("row", "col"), None),
        P(("row", "col")),
        P(("row", "col")),
    )
    out_specs = (P(None, "row", "col"), P(), P(("row", "col"), None), P(("row", "col"), None))
    return jax.shard_map(
        on_device, mesh=mesh, in_specs=in_specs, out_specs=out_specs, check_vma=False
    )
```
